32 devices in a mesh: grp: 8 (over y, x, core), tp: 4 (over z).
Axes of the slice: x: 2, y: 2, z: 4, core: 2. Of those that a mesh axis runs over, the one named last changes fastest.
Arguments:
- tokens: bfloat16 [4096, 6144], P('grp'), may hold values from -40 to 40
- norm_gain: bfloat16 [6144], replicated, may hold values from 0.099609375 to 1.8984375
- up_weight: bfloat16 [6144, 12288], P('grp', 'tp'), may hold values from -0.078125 to 0.078125
- up_bias: float32 [12288], P('tp'), may hold values from -3 to 3
- down_weight: bfloat16 [12288, 6144], P('tp', 'grp'), may hold values from -0.0546875 to 0.0546875
- down_bias: float32 [6144], P('tp'), may hold values from -2 to 2
Outputs:
- encoded: bfloat16 [4096, 6144], P('grp', 'tp')
The draws below stay inside these ranges and needn't reach their ends.
All inputs are finite; a program needn't handle non-finite values.
Results may differ from the reference program's by a relative error of at most 0.0085.
Values may be sent and summed in bfloat16 or wider, within the bound.
A program may use at most 128 MiB of HBM per device.

```python
import jax
import jax.numpy as jnp
from jax import lax

D = 6144
FF = 12288
ROWS = 4096
N_TP = 4


def draw_tokens(key, part):
    keys = jax.random.split(key, 4)
    offsets = jax.random.uniform(keys[0], (16,), jnp.float32, -0.5, 0.5)
    column = jax.random.uniform(keys[1], (D,), jnp.float32, -0.5, 0.5) + jnp.repeat(offsets, D // 16)
    column_scale = 10.0 ** column
    row_scale = jnp.exp(jax.random.uniform(keys[2], (ROWS, 1), jnp.float32, -0.69, 0.69))
    base = jnp.clip(jax.random.normal(keys[3], (ROWS, D), jnp.float32), -6.0, 6.0)
    return jnp.clip(base * column_scale * row_scale, -40.0, 40.0).astype(jnp.bfloat16)


def block_scale(own_key, extent, pieces, low, largest):
    loudness, own = 1.0, jax.random.fold_in(own_key, 6)
    for dim, shards_of in pieces:
        steps = jnp.exp(jax.random.uniform(jax.random.fold_in(own, dim), (shards_of,), jnp.float32, low / len(pieces), largest / len(pieces)))
        loudness = loudness * jnp.repeat(steps, extent[dim] // shards_of).reshape([-1 if axis == dim else 1 for axis in range(len(extent))])
    return loudness


def bell_draw(rng, shape, spread, bound, shards=(), held_as=jnp.bfloat16):
    array = spread * jax.random.normal(rng, shape, jnp.float32)
    if shards:
        array = array * block_scale(rng, shape, shards, -0.22, 0.18)
    return jnp.clip(array, -bound, bound).astype(held_as)


def setup_inputs(seed: int = 0) -> dict:
    key_list = jax.random.split(jax.random.key(seed), 7)
    return {
        "tokens": draw_tokens(jax.random.fold_in(key_list[6], 71), 0),
        "norm_gain": jnp.clip(1.0 + 0.18 * jax.random.normal(key_list[1], (D,), jnp.float32), 0.099609375, 1.8984375).astype(jnp.bfloat16),
        "up_weight": bell_draw(key_list[2], (D, FF), D ** -0.5, 0.078125, ((0, 8), (1, 4))),
        "up_bias": bell_draw(key_list[3], (FF,), 0.5, 3.0, ((0, 4),), jnp.float32),
        "down_weight": bell_draw(key_list[4], (FF, D), FF ** -0.5, 0.0546875, ((0, 4), (1, 8))),
        "down_bias": bell_draw(key_list[5], (D,), 0.3, 2.0, ((0, 4),), jnp.float32),
    }


def reference(tokens, norm_gain, up_weight, up_bias, down_weight, down_bias):
    values = tokens.astype(jnp.float32)
    centre = lax.optimization_barrier(jnp.mean(values, axis=1, keepdims=True))
    shifted = values - centre
    variance = lax.optimization_barrier(jnp.mean(shifted * shifted, axis=1, keepdims=True))
    normed = (shifted * lax.rsqrt(variance + 1e-06) * norm_gain.astype(jnp.float32)).astype(jnp.bfloat16)
    pre = jnp.dot(normed, up_weight, preferred_element_type=jnp.float32) + up_bias
    hidden = jax.nn.gelu(pre, approximate=True).astype(jnp.bfloat16)
    width = FF // N_TP
    summed = jnp.zeros(values.shape, jnp.float32)
    for index in range(N_TP):
        term = jnp.dot(hidden[:, index * width:(index + 1) * width], down_weight[index * width:(index + 1) * width, :], preferred_element_type=jnp.float32)
        rounded = lax.optimization_barrier(term.astype(jnp.bfloat16))
        summed = summed + rounded.astype(jnp.float32)
    return (values + summed + down_bias).astype(jnp.bfloat16)
```

```python
import functools

import jax
import jax.numpy as jnp
from jax import lax
from jax.experimental import pallas as pl
from jax.experimental.pallas import tpu as pltpu
from jax.sharding import PartitionSpec as P

MESH = pl.DeviceIdType.MESH
HID_CHUNK = 512
COL_CHUNK = 128
EARLY_V = 2


def chunk_of(extent, wanted):
    step = min(wanted, extent)
    while extent % step:
        step -= 128
    return step


def dot(a, b):
    return jnp.dot(a, b, preferred_element_type=jnp.float32)


def build(groups, planes):
    bits = groups.bit_length() - 1
    k_bit, n_bit = bits - 1, 1
    up_bits = [b for b in range(1, bits) if b != k_bit] + [0]
    down_bits = [b for b in range(bits - 1, 0, -1) if b != n_bit] + [0]
    per_plane = groups // planes
    pieces = groups // 2
    slots = planes // 2

    def masks_of(order):
        masks = [()]
        for bit in order:
            masks = masks + [m + (bit,) for m in masks]
        return masks

    up_masks, down_masks = masks_of(up_bits), masks_of(down_bits)

    def stages_from(piece, order):
        return [s for s in range(len(order)) if (1 << s) > piece]

    def kernel(
        tok, gain, w, ubias, v, dbias, out, vh,
        tk, sh, xo, xp, wb, ps, pr, acc, hid, hx, zu, zd, fr, ob, *rest,
    ):
        rest = list(rest)
        vb = rest.pop(0) if len(rest) == 26 else wb
        (gv, ub, db, tk_sem, misc_sem, wl_sem, vl_sem,
         up_send, up_recv, dn_send, dn_recv, x_send, x_recv,
         zxu_send, zxu_recv, zxd_send, zxd_recv,
         p_send, p_recv, h_send, h_recv, z_send, zu_recv, zd_recv, f_sem) = rest
        f_send, f_recv = f_sem.at[0], f_sem.at[1]

        me = lax.axis_index("grp")
        z = lax.axis_index("tp")
        rows, width = tok.shape
        depth, hidden = w.shape
        out_block = v.shape[1]
        own_width = out.shape[1]
        half = width // 2
        chunks, _, hj = wb.shape
        cols = vb.shape[2] // pieces
        col_chunks = vb.shape[0]
        slot_width = per_plane * cols
        shard = rows // planes

        def bit_of(b):
            return (me // (1 << b)) % 2

        def flipped(index_bits):
            index = me
            for b in index_bits:
                index = index + (1 - 2 * bit_of(b)) * (1 << b)
            return index

        def near(b):
            return {"grp": flipped((b,))}

        k_half, n_half = bit_of(k_bit), bit_of(n_bit)

        def up_place(mask):
            return pl.multiple_of((flipped(mask) % pieces) * depth, depth)

        def down_place(mask):
            block = flipped(mask)
            return pl.multiple_of(((block // 4) * 2 + block % 2) * cols, cols)

        def up_copy(j, piece, stage):
            place = pl.ds(up_place(up_masks[piece]), depth)
            landing = wb.at[j, place, :]
            source = w.at[:, pl.ds(pl.multiple_of(j * hj, hj), hj)] if piece == 0 else landing
            slot = piece + (1 << stage) - 1
            return pltpu.make_async_remote_copy(
                src_ref=source, dst_ref=landing,
                send_sem=up_send.at[j, slot], recv_sem=up_recv.at[j, slot],
                device_id=near(up_bits[stage]), device_id_type=MESH)

        def up_arrival(j, piece):
            place = pl.ds(up_place(up_masks[piece]), depth)
            landing = wb.at[j, place, :]
            stage = piece.bit_length() - 1
            return pltpu.make_async_remote_copy(
                src_ref=landing, dst_ref=landing,
                send_sem=up_send.at[j, piece - 1], recv_sem=up_recv.at[j, piece - 1],
                device_id=near(up_bits[stage]), device_id_type=MESH)

        def w_local(j):
            return pltpu.make_async_copy(
                w.at[:, pl.ds(pl.multiple_of(j * hj, hj), hj)],
                wb.at[j, pl.ds(up_place(()), depth), :], wl_sem.at[j])

        def down_copy(q, piece, stage):
            place = pl.ds(down_place(down_masks[piece]), cols)
            landing = vh.at[q, :, place]
            source = v.at[:, pl.ds(pl.multiple_of(q * cols, cols), cols)] if piece == 0 else landing
            slot = piece + (1 << stage) - 1
            return pltpu.make_async_remote_copy(
                src_ref=source, dst_ref=landing,
                send_sem=dn_send.at[q, slot], recv_sem=dn_recv.at[q, slot],
                device_id=near(down_bits[stage]), device_id_type=MESH)

        def down_arrival(q, piece):
            landing = vh.at[q, :, pl.ds(down_place(down_masks[piece]), cols)]
            stage = piece.bit_length() - 1
            return pltpu.make_async_remote_copy(
                src_ref=landing, dst_ref=landing,
                send_sem=dn_send.at[q, piece - 1], recv_sem=dn_recv.at[q, piece - 1],
                device_id=near(down_bits[stage]), device_id_type=MESH)

        def v_local(q, piece):
            place = pl.ds(down_place(down_masks[piece]), cols)
            source = v.at[:, pl.ds(pl.multiple_of(q * cols, cols), cols)] if piece == 0 else vh.at[q, :, place]
            return pltpu.make_async_copy(source, vb.at[q, :, place], vl_sem.at[q, piece])

        barrier = pltpu.get_barrier_semaphore()
        for b in range(bits):
            pl.semaphore_signal(barrier, inc=1, device_id=near(b), device_id_type=MESH)

        @pl.when(z > 0)
        def _():
            pl.semaphore_signal(barrier, inc=1, device_id={"tp": z - 1}, device_id_type=MESH)

        @pl.when(z < planes - 1)
        def _():
            pl.semaphore_signal(barrier, inc=1, device_id={"tp": z + 1}, device_id_type=MESH)

        shard_rows = pl.ds(pl.multiple_of(z * shard, shard), shard)

        def token_copy(index, slot):
            source = shard_rows if index < 0 else pl.ds(index * shard, shard)
            return pltpu.make_async_copy(tok.at[source, :], tk.at[slot], tk_sem.at[slot])

        token_copy(-1, 0).start()
        token_copy(0, 1).start()
        small = [
            pltpu.make_async_copy(gain, gv, misc_sem.at[0]),
            pltpu.make_async_copy(ubias, ub, misc_sem.at[1]),
            pltpu.make_async_copy(dbias, db, misc_sem.at[2]),
            pltpu.make_async_copy(
                tok.at[:, pl.ds(pl.multiple_of(z * own_width, own_width), own_width)], ob, misc_sem.at[3]),
        ]
        for copy in small:
            copy.start()

        neighbours = bits + jnp.where(z > 0, 1, 0) + jnp.where(z < planes - 1, 1, 0)
        pl.semaphore_wait(barrier, neighbours)

        def start_up(j, carry):
            for stage in range(len(up_bits)):
                up_copy(j, 0, stage).start()
            w_local(j).start()
            return carry

        lax.fori_loop(0, chunks, start_up, 0)
        small[0].wait()

        tile = 16

        def normalise(slot, column, dst, base):
            def body(i, carry):
                at = pl.multiple_of(i * tile, tile)
                values = tk[slot, pl.ds(at, tile), :].astype(jnp.float32)
                centre = jnp.mean(values, axis=1, keepdims=True)
                shifted = values - centre
                scale = lax.rsqrt(jnp.mean(shifted * shifted, axis=1, keepdims=True) + 1e-06)
                part = tk[slot, pl.ds(at, tile), pl.ds(column, half)].astype(jnp.float32)
                normed = (part - centre) * scale * gv[:, pl.ds(column, half)].astype(jnp.float32)
                dst[pl.ds(pl.multiple_of(base + at, tile), tile), :] = normed.astype(jnp.bfloat16)
                return carry

            lax.fori_loop(0, shard // tile, body, 0)

        own_column = pl.multiple_of(k_half * half, half)
        other_column = pl.multiple_of((1 - k_half) * half, half)

        token_copy(-1, 0).wait()
        normalise(0, other_column, sh, 0)
        shard_send = pltpu.make_async_remote_copy(
            src_ref=sh, dst_ref=xp.at[shard_rows, :],
            send_sem=x_send, recv_sem=x_recv, device_id=near(k_bit), device_id_type=MESH)
        shard_send.start()

        def start_down(q):
            down_copy(q, 0, 0).start()

        early = min(EARLY_V, col_chunks)
        for q in range(early):
            start_down(q)

        def start_down_core(q, carry):
            for stage in range(1, len(down_bits)):
                down_copy(q, 0, stage).start()
            return carry

        for c in range(planes):
            slot = (c + 1) % 2
            if c + 1 < planes:
                token_copy(c + 1, 1 - slot).start()
            token_copy(c, slot).wait()
            normalise(slot, own_column, xo, c * shard)

        shard_send.wait_recv()

        def pass_on(distance, rising):
            source = z - distance if rising else z + distance
            place = pl.ds(pl.multiple_of(source * shard, shard), shard)
            return pltpu.make_async_remote_copy(
                src_ref=xp.at[place, :], dst_ref=xp.at[place, :],
                send_sem=(zxu_send if rising else zxd_send).at[distance],
                recv_sem=(zxu_recv if rising else zxd_recv).at[distance],
                device_id={"tp": z + 1 if rising else z - 1}, device_id_type=MESH)

        def arrival(distance, rising):
            source = z - distance if rising else z + distance
            place = pl.ds(pl.multiple_of(source * shard, shard), shard)
            return pltpu.make_async_remote_copy(
                src_ref=xp.at[place, :], dst_ref=xp.at[place, :],
                send_sem=(zxu_send if rising else zxd_send).at[distance - 1],
                recv_sem=(zxu_recv if rising else zxd_recv).at[distance - 1],
                device_id={"tp": z - 1 if rising else z + 1}, device_id_type=MESH)

        for distance in range(planes):
            if distance:
                @pl.when(z >= distance)
                def _():
                    arrival(distance, True).wait_recv()

                @pl.when(z + distance <= planes - 1)
                def _():
                    arrival(distance, False).wait_recv()

            if distance < planes - 1:
                @pl.when((z >= distance) & (z < planes - 1))
                def _():
                    pass_on(distance, True).start()

                @pl.when((z + distance <= planes - 1) & (z > 0))
                def _():
                    pass_on(distance, False).start()

        shard_send.wait_send()
        small[1].wait()

        row_tile = min(256, rows)
        row_tiles = rows // row_tile

        def partial_copy(j):
            return pltpu.make_async_remote_copy(
                src_ref=ps.at[j, :, pl.ds(0, hj)], dst_ref=pr.at[j], send_sem=p_send.at[j], recv_sem=p_recv.at[j],
                device_id=near(k_bit), device_id_type=MESH)

        def hidden_copy(j):
            place = pl.ds(pl.multiple_of(j * hj, hj), hj)
            return pltpu.make_async_remote_copy(
                src_ref=hid.at[:, place], dst_ref=hx.at[:, place], send_sem=h_send.at[j], recv_sem=h_recv.at[j],
                device_id=near(n_bit), device_id_type=MESH)

        def finish(j):
            partial_copy(j).wait_recv()
            place = pl.ds(pl.multiple_of(j * hj, hj), hj)

            def body(i, carry):
                at = pl.ds(pl.multiple_of(i * 64, 64), 64)
                pre = acc[j % 2, at, pl.ds(0, hj)] + pr[j, at, :].astype(jnp.float32) + ub[:, place]
                hid[at, place] = jax.nn.gelu(pre, approximate=True).astype(jnp.bfloat16)
                return carry

            lax.fori_loop(0, rows // 64, body, 0)
            hidden_copy(j).start()

        def up_step(j, carry):
            for piece in range(1, pieces):
                stages = stages_from(piece, up_bits)
                if stages:
                    up_arrival(j, piece).wait_recv()
                    for stage in stages:
                        up_copy(j, piece, stage).start()

            @pl.when(j > 0)
            def _():
                finish(j - 1)

            for piece in range(1, pieces):
                if not stages_from(piece, up_bits):
                    up_arrival(j, piece).wait_recv()
            w_local(j).wait()

            def sent(i, carry):
                at = pl.ds(pl.multiple_of(i * row_tile, row_tile), row_tile)
                ps[j, at, pl.ds(0, hj)] = dot(xp[at, :], wb[j]).astype(jnp.bfloat16)
                return carry

            lax.fori_loop(0, row_tiles, sent, 0)
            partial_copy(j).start()

            def kept(i, carry):
                at = pl.ds(pl.multiple_of(i * row_tile, row_tile), row_tile)
                acc[j % 2, at, pl.ds(0, hj)] = dot(xo[at, :], wb[j])
                return carry

            lax.fori_loop(0, row_tiles, kept, 0)
            return carry

        lax.fori_loop(0, chunks, up_step, 0)
        for q in range(early, col_chunks):
            start_down(q)
        lax.fori_loop(0, col_chunks, start_down_core, 0)
        finish(chunks - 1)

        def settle_up(j, carry):
            for piece in range(pieces):
                for stage in stages_from(piece, up_bits):
                    up_copy(j, piece, stage).wait_send()
            partial_copy(j).wait_send()
            return carry

        lax.fori_loop(0, chunks, settle_up, 0)
        small[2].wait()
        small[3].wait()

        def target(u):
            return 2 * u + n_half

        def z_up(item, q, u):
            return pltpu.make_async_remote_copy(
                src_ref=ps.at[q, :, pl.ds(u * slot_width, slot_width)], dst_ref=zu.at[item, u],
                send_sem=z_send.at[item, u], recv_sem=zu_recv.at[item, u],
                device_id={"tp": z + 1}, device_id_type=MESH)

        def z_down(item, q, u):
            return pltpu.make_async_remote_copy(
                src_ref=ps.at[q, :, pl.ds(u * slot_width, slot_width)], dst_ref=zd.at[item, u],
                send_sem=z_send.at[item, u], recv_sem=zd_recv.at[item, u],
                device_id={"tp": z - 1}, device_id_type=MESH)

        def final_copy(q, u):
            return pltpu.make_async_remote_copy(
                src_ref=ps.at[q, :, pl.ds(u * slot_width, slot_width)], dst_ref=fr.at[q],
                send_sem=f_send.at[q], recv_sem=f_recv.at[q],
                device_id=near(n_bit), device_id_type=MESH)

        def deliver(q, value_of):
            for c in range(per_plane):
                place = pl.ds(pl.multiple_of(c * out_block + q * cols, cols), cols)

                def body(i, carry):
                    at = pl.ds(pl.multiple_of(i * 64, 64), 64)
                    total = ob[at, place].astype(jnp.float32) + value_of(at, c) + db[:, place]
                    ob[at, place] = total.astype(jnp.bfloat16)
                    return carry

                lax.fori_loop(0, rows // 64, body, 0)

        def chain(item, q, mine):
            buf = item % 2
            for u in range(slots):
                to = target(u)
                lanes = pl.ds(u * slot_width, slot_width)

                @pl.when((z > 0) & (z <= to))
                def _():
                    z_up(item, q, u).wait_recv()
                    acc[buf, :, lanes] = acc[buf, :, lanes] + zu[item, u].astype(jnp.float32)

                @pl.when((z < planes - 1) & (z >= to))
                def _():
                    z_down(item, q, u).wait_recv()
                    acc[buf, :, lanes] = acc[buf, :, lanes] + zd[item, u].astype(jnp.float32)

                @pl.when(z != to)
                def _():
                    if not mine:
                        z_up(item - col_chunks, q, u).wait_send()
                    ps[q, :, lanes] = acc[buf, :, lanes].astype(jnp.bfloat16)

                @pl.when(z < to)
                def _():
                    z_up(item, q, u).start()

                @pl.when(z > to)
                def _():
                    z_down(item, q, u).start()

                @pl.when(z == to)
                def _():
                    if mine:
                        deliver(q, lambda at, c: acc[buf, at, pl.ds(u * slot_width + c * cols, cols)])
                    else:
                        ps[q, :, lanes] = acc[buf, :, lanes].astype(jnp.bfloat16)
                        final_copy(q, u).start()

        def down_dot(src, item, q):
            def body(i, carry):
                at = pl.ds(pl.multiple_of(i * row_tile, row_tile), row_tile)
                acc[item % 2, at, pl.ds(0, cols * pieces)] = dot(src[at, :], vb[q])
                return carry

            lax.fori_loop(0, row_tiles, body, 0)

        def own_step(q, carry):
            for piece in range(1, pieces):
                stages = stages_from(piece, down_bits)
                if stages:
                    down_arrival(q, piece).wait_recv()
                    for stage in stages:
                        down_copy(q, piece, stage).start()
                    v_local(q, piece).start()
            v_local(q, 0).start()

            @pl.when(q > 0)
            def _():
                chain(q - 1, q - 1, True)

            for piece in range(1, pieces):
                if not stages_from(piece, down_bits):
                    down_arrival(q, piece).wait_recv()
                    v_local(q, piece).start()
            for piece in range(pieces):
                v_local(q, piece).wait()
            down_dot(hid, q, q)
            return carry

        lax.fori_loop(0, col_chunks, own_step, 0)
        chain(col_chunks - 1, col_chunks - 1, True)

        def hidden_arrives(j, carry):
            hidden_copy(j).wait_recv()
            return carry

        lax.fori_loop(0, chunks, hidden_arrives, 0)

        def other_step(q, carry):
            down_dot(hx, col_chunks + q, q)

            @pl.when(q > 0)
            def _():
                chain(col_chunks + q - 1, q - 1, False)
            return carry

        lax.fori_loop(0, col_chunks, other_step, 0)
        chain(2 * col_chunks - 1, col_chunks - 1, False)

        @pl.when(z % 2 != n_half)
        def _():
            def body(q, carry):
                final_copy(q, 0).wait_recv()
                deliver(q, lambda at, c: fr[q, at, pl.ds(c * cols, cols)].astype(jnp.float32))
                return carry

            lax.fori_loop(0, col_chunks, body, 0)

        write = pltpu.make_async_copy(ob, out, misc_sem.at[0])
        write.start()

        def settle_down(q, carry):
            for piece in range(pieces):
                for stage in stages_from(piece, down_bits):
                    down_copy(q, piece, stage).wait_send()
            for u in range(slots):
                @pl.when(z != target(u))
                def _():
                    z_up(col_chunks + q, q, u).wait_send()

                @pl.when(z == target(u))
                def _():
                    final_copy(q, u).wait_send()
            return carry

        lax.fori_loop(0, col_chunks, settle_down, 0)

        def settle_hidden(j, carry):
            hidden_copy(j).wait_send()
            return carry

        lax.fori_loop(0, chunks, settle_hidden, 0)
        for distance in range(planes - 1):
            @pl.when((z >= distance) & (z < planes - 1))
            def _():
                pass_on(distance, True).wait_send()

            @pl.when((z + distance <= planes - 1) & (z > 0))
            def _():
                pass_on(distance, False).wait_send()
        write.wait()

    def per_device(tokens, norm_gain, up_weight, up_bias, down_weight, down_bias):
        rows, width = tokens.shape
        depth, hidden = up_weight.shape
        out_block = down_weight.shape[1]
        own_width = down_bias.shape[0]
        hj = chunk_of(hidden, HID_CHUNK)
        cols = chunk_of(out_block, COL_CHUNK)
        chunks, col_chunks = hidden // hj, out_block // cols
        half, shard = width // 2, rows // planes
        slab = cols * pieces
        bf, f32 = jnp.bfloat16, jnp.float32
        dma = pltpu.SemaphoreType.DMA
        shared = (chunks, half, hj) == (col_chunks, hidden, slab)
        scratch = [
            pltpu.VMEM((2, shard, width), bf),
            pltpu.VMEM((shard, half), bf),
            pltpu.VMEM((rows, half), bf),
            pltpu.VMEM((rows, half), bf),
            pltpu.VMEM((chunks, half, hj), bf),
            pltpu.VMEM((max(chunks, col_chunks), rows, max(hj, slab)), bf),
            pltpu.VMEM((chunks, rows, hj), bf),
            pltpu.VMEM((2, rows, max(hj, slab)), f32),
            pltpu.VMEM((rows, hidden), bf),
            pltpu.VMEM((rows, hidden), bf),
            pltpu.VMEM((2 * col_chunks, slots, rows, per_plane * cols), bf),
            pltpu.VMEM((2 * col_chunks, slots, rows, per_plane * cols), bf),
            pltpu.VMEM((col_chunks, rows, per_plane * cols), bf),
            pltpu.VMEM((rows, own_width), bf),
        ]
        if not shared:
            scratch.append(pltpu.VMEM((col_chunks, hidden, slab), bf))
        scratch += [
            pltpu.VMEM((1, width), bf),
            pltpu.VMEM((1, hidden), f32),
            pltpu.VMEM((1, own_width), f32),
            dma((2,)), dma((4,)), dma((chunks,)), dma((col_chunks, pieces)),
            dma((chunks, pieces - 1)), dma((chunks, pieces - 1)),
            dma((col_chunks, pieces - 1)), dma((col_chunks, pieces - 1)),
            dma, dma,
            dma((planes,)), dma((planes,)), dma((planes,)), dma((planes,)),
            dma((chunks,)), dma((chunks,)), dma((chunks,)), dma((chunks,)),
            dma((2 * col_chunks, slots)), dma((2 * col_chunks, slots)), dma((2 * col_chunks, slots)),
            dma((2, col_chunks)),
        ]
        hbm = pl.BlockSpec(memory_space=pltpu.HBM)
        result, _ = pl.pallas_call(
            kernel,
            out_shape=(
                jax.ShapeDtypeStruct((rows, own_width), bf),
                jax.ShapeDtypeStruct((col_chunks, hidden, slab), bf),
            ),
            in_specs=[hbm] * 6,
            out_specs=(hbm, hbm),
            scratch_shapes=scratch,
            compiler_params=pltpu.CompilerParams(
                collective_id=0, has_side_effects=True, vmem_limit_bytes=67043328),
        )(tokens, norm_gain[None, :], up_weight, up_bias[None, :], down_weight, down_bias[None, :])
        return result

    return per_device


def solution(mesh):
    in_specs = (P("grp", None), P(), P("grp", "tp"), P("tp"), P("tp", "grp"), P("tp"))
    return jax.shard_map(
        build(mesh.shape["grp"], mesh.shape["tp"]),
        mesh=mesh, in_specs=in_specs, out_specs=P("grp", "tp"), check_vma=False,
    )
```

```python
import functools

import jax
import jax.numpy as jnp
from jax import lax
from jax.experimental import pallas as pl
from jax.experimental.pallas import tpu as pltpu
from jax.sharding import PartitionSpec as P

MESH = pl.DeviceIdType.MESH
HID_CHUNK = 512
COL_CHUNK = 128
ROW_SPLIT = 2
EARLY_V = (-1, 1)


def chunk_of(extent, wanted):
    step = min(wanted, extent)
    while extent % step:
        step -= 128
    return step


def dot(a, b):
    return jnp.dot(a, b, preferred_element_type=jnp.float32)


def build(groups, planes):
    bits = groups.bit_length() - 1
    k_bit, n_bit = bits - 1, 1
    up_bits = [b for b in range(1, bits) if b != k_bit] + [0]
    down_bits = [b for b in range(bits - 1, 0, -1) if b != n_bit] + [0]
    per_plane = groups // planes
    pieces = groups // 2
    slots = planes // 2

    def masks_of(order):
        masks = [()]
        for bit in order:
            masks = masks + [m + (bit,) for m in masks]
        return masks

    up_masks, down_masks = masks_of(up_bits), masks_of(down_bits)

    def stages_from(piece, order):
        return [s for s in range(len(order)) if (1 << s) > piece]

    def kernel(
        tok, gain, w, ubias, v, dbias, out, vh,
        tk, sh, xo, xp, wb, ps, pr, acc, hid, hx, zu, zd, fr, cr, ob, *rest,
    ):
        rest = list(rest)
        vb = rest.pop(0) if len(rest) == 27 else wb
        (gv, ub, db, tk_sem, misc_sem, wl_sem, vl_sem,
         up_send, up_recv, dn_send, dn_recv, x_send, x_recv,
         zxu_send, zxu_recv, zxd_send, zxd_recv,
         p_send, p_recv, h_send, h_recv, z_send, zu_recv, zd_recv, f_sem, c_sem) = rest
        f_send, f_recv, c_send, c_recv = f_sem.at[0], f_sem.at[1], c_sem.at[0], c_sem.at[1]

        me = lax.axis_index("grp")
        z = lax.axis_index("tp")
        rows, width = tok.shape
        depth, hidden = w.shape
        out_block = v.shape[1]
        own_width = out.shape[1]
        half = width // 2
        chunks, _, hj = wb.shape
        cols = vb.shape[2] // pieces
        col_chunks = vb.shape[0]
        slot_width = per_plane * cols
        shard = rows // planes

        def bit_of(b):
            return (me // (1 << b)) % 2

        def flipped(index_bits):
            index = me
            for b in index_bits:
                index = index + (1 - 2 * bit_of(b)) * (1 << b)
            return index

        def near(b):
            return {"grp": flipped((b,))}

        k_half, n_half = bit_of(k_bit), bit_of(n_bit)

        def up_place(mask):
            return pl.multiple_of((flipped(mask) % pieces) * depth, depth)

        def down_place(mask):
            block = flipped(mask)
            return pl.multiple_of(((block // 4) * 2 + block % 2) * cols, cols)

        def up_copy(j, piece, stage):
            place = pl.ds(up_place(up_masks[piece]), depth)
            landing = wb.at[j, place, :]
            source = w.at[:, pl.ds(pl.multiple_of(j * hj, hj), hj)] if piece == 0 else landing
            slot = piece + (1 << stage) - 1
            return pltpu.make_async_remote_copy(
                src_ref=source, dst_ref=landing,
                send_sem=up_send.at[j, slot], recv_sem=up_recv.at[j, slot],
                device_id=near(up_bits[stage]), device_id_type=MESH)

        def up_arrival(j, piece):
            place = pl.ds(up_place(up_masks[piece]), depth)
            landing = wb.at[j, place, :]
            stage = piece.bit_length() - 1
            return pltpu.make_async_remote_copy(
                src_ref=landing, dst_ref=landing,
                send_sem=up_send.at[j, piece - 1], recv_sem=up_recv.at[j, piece - 1],
                device_id=near(up_bits[stage]), device_id_type=MESH)

        def w_local(j):
            return pltpu.make_async_copy(
                w.at[:, pl.ds(pl.multiple_of(j * hj, hj), hj)],
                wb.at[j, pl.ds(up_place(()), depth), :], wl_sem.at[j])

        def down_copy(q, piece, stage):
            place = pl.ds(down_place(down_masks[piece]), cols)
            landing = vh.at[q, :, place]
            source = v.at[:, pl.ds(pl.multiple_of(q * cols, cols), cols)] if piece == 0 else landing
            slot = piece + (1 << stage) - 1
            return pltpu.make_async_remote_copy(
                src_ref=source, dst_ref=landing,
                send_sem=dn_send.at[q, slot], recv_sem=dn_recv.at[q, slot],
                device_id=near(down_bits[stage]), device_id_type=MESH)

        def down_arrival(q, piece):
            landing = vh.at[q, :, pl.ds(down_place(down_masks[piece]), cols)]
            stage = piece.bit_length() - 1
            return pltpu.make_async_remote_copy(
                src_ref=landing, dst_ref=landing,
                send_sem=dn_send.at[q, piece - 1], recv_sem=dn_recv.at[q, piece - 1],
                device_id=near(down_bits[stage]), device_id_type=MESH)

        def v_local(q, piece):
            place = pl.ds(down_place(down_masks[piece]), cols)
            source = v.at[:, pl.ds(pl.multiple_of(q * cols, cols), cols)] if piece == 0 else vh.at[q, :, place]
            return pltpu.make_async_copy(source, vb.at[q, :, place], vl_sem.at[q, piece])

        barrier = pltpu.get_barrier_semaphore()
        for b in range(bits):
            pl.semaphore_signal(barrier, inc=1, device_id=near(b), device_id_type=MESH)

        @pl.when(z > 0)
        def _():
            pl.semaphore_signal(barrier, inc=1, device_id={"tp": z - 1}, device_id_type=MESH)

        @pl.when(z < planes - 1)
        def _():
            pl.semaphore_signal(barrier, inc=1, device_id={"tp": z + 1}, device_id_type=MESH)

        shard_rows = pl.ds(pl.multiple_of(z * shard, shard), shard)

        def token_copy(index, slot):
            source = shard_rows if index < 0 else pl.ds(index * shard, shard)
            return pltpu.make_async_copy(tok.at[source, :], tk.at[slot], tk_sem.at[slot])

        token_copy(-1, 0).start()
        token_copy(0, 1).start()
        small = [
            pltpu.make_async_copy(gain, gv, misc_sem.at[0]),
            pltpu.make_async_copy(ubias, ub, misc_sem.at[1]),
            pltpu.make_async_copy(dbias, db, misc_sem.at[2]),
            pltpu.make_async_copy(
                tok.at[:, pl.ds(pl.multiple_of(z * own_width, own_width), own_width)], ob, misc_sem.at[3]),
        ]
        for copy in small:
            copy.start()

        neighbours = bits + jnp.where(z > 0, 1, 0) + jnp.where(z < planes - 1, 1, 0)
        pl.semaphore_wait(barrier, neighbours)

        def start_up(j, carry):
            for stage in range(len(up_bits)):
                up_copy(j, 0, stage).start()
            w_local(j).start()
            return carry

        lax.fori_loop(0, chunks, start_up, 0)
        small[0].wait()

        tile = 16

        def normalise(slot, column, dst, base):
            def body(i, carry):
                at = pl.multiple_of(i * tile, tile)
                values = tk[slot, pl.ds(at, tile), :].astype(jnp.float32)
                centre = jnp.mean(values, axis=1, keepdims=True)
                shifted = values - centre
                scale = lax.rsqrt(jnp.mean(shifted * shifted, axis=1, keepdims=True) + 1e-06)
                part = tk[slot, pl.ds(at, tile), pl.ds(column, half)].astype(jnp.float32)
                normed = (part - centre) * scale * gv[:, pl.ds(column, half)].astype(jnp.float32)
                dst[pl.ds(pl.multiple_of(base + at, tile), tile), :] = normed.astype(jnp.bfloat16)
                return carry

            lax.fori_loop(0, shard // tile, body, 0)

        own_column = pl.multiple_of(k_half * half, half)
        other_column = pl.multiple_of((1 - k_half) * half, half)

        token_copy(-1, 0).wait()
        normalise(0, other_column, sh, 0)
        shard_send = pltpu.make_async_remote_copy(
            src_ref=sh, dst_ref=xp.at[shard_rows, :],
            send_sem=x_send, recv_sem=x_recv, device_id=near(k_bit), device_id_type=MESH)
        shard_send.start()

        def start_down(q):
            down_copy(q, 0, 0).start()

        early = [q for q in range(len(EARLY_V)) if q < col_chunks]
        for q in early:
            if EARLY_V[q] < 0:
                start_down(q)

        def start_down_core(q, carry):
            for stage in range(1, len(down_bits)):
                down_copy(q, 0, stage).start()
            return carry

        for c in range(planes):
            slot = (c + 1) % 2
            if c + 1 < planes:
                token_copy(c + 1, 1 - slot).start()
            token_copy(c, slot).wait()
            normalise(slot, own_column, xo, c * shard)

        def pass_on(distance, rising):
            source = z - distance if rising else z + distance
            place = pl.ds(pl.multiple_of(source * shard, shard), shard)
            return pltpu.make_async_remote_copy(
                src_ref=xp.at[place, :], dst_ref=xp.at[place, :],
                send_sem=(zxu_send if rising else zxd_send).at[distance],
                recv_sem=(zxu_recv if rising else zxd_recv).at[distance],
                device_id={"tp": z + 1 if rising else z - 1}, device_id_type=MESH)

        def arrival(distance, rising):
            source = z - distance if rising else z + distance
            place = pl.ds(pl.multiple_of(source * shard, shard), shard)
            return pltpu.make_async_remote_copy(
                src_ref=xp.at[place, :], dst_ref=xp.at[place, :],
                send_sem=(zxu_send if rising else zxd_send).at[distance - 1],
                recv_sem=(zxu_recv if rising else zxd_recv).at[distance - 1],
                device_id={"tp": z - 1 if rising else z + 1}, device_id_type=MESH)

        def pass_tokens(distance):
            @pl.when(distance == 0)
            def _():
                shard_send.wait_recv()

            @pl.when((distance > 0) & (z >= distance))
            def _():
                arrival(distance, True).wait_recv()

            @pl.when((distance > 0) & (z + distance <= planes - 1))
            def _():
                arrival(distance, False).wait_recv()

            @pl.when((z >= distance) & (z < planes - 1) & (distance < planes - 1))
            def _():
                pass_on(distance, True).start()

            @pl.when((z + distance <= planes - 1) & (z > 0) & (distance < planes - 1))
            def _():
                pass_on(distance, False).start()

        small[1].wait()

        def partial_copy(j, block):
            place = pl.ds(pl.multiple_of(block * shard, shard), shard)
            return pltpu.make_async_remote_copy(
                src_ref=ps.at[j, place, pl.ds(0, hj)], dst_ref=pr.at[j, place, :],
                send_sem=p_send.at[j, block], recv_sem=p_recv.at[j, block],
                device_id=near(k_bit), device_id_type=MESH)

        def hidden_copy(j):
            place = pl.ds(pl.multiple_of(j * hj, hj), hj)
            return pltpu.make_async_remote_copy(
                src_ref=hid.at[:, place], dst_ref=hx.at[:, place], send_sem=h_send.at[j], recv_sem=h_recv.at[j],
                device_id=near(n_bit), device_id_type=MESH)

        row_tile = min(256, rows)

        def finish(j):
            place = pl.ds(pl.multiple_of(j * hj, hj), hj)

            def kept(i, carry):
                at = pl.ds(pl.multiple_of(i * row_tile, row_tile), row_tile)
                acc[at, :] = dot(xo[at, :], wb[j])
                return carry

            lax.fori_loop(0, rows // row_tile, kept, 0)
            for block in range(planes):
                partial_copy(j, block).wait_recv()

            def body(i, carry):
                at = pl.ds(pl.multiple_of(i * 64, 64), 64)
                pre = acc[at, :] + pr[j, at, :].astype(jnp.float32) + ub[:, place]
                hid[at, place] = jax.nn.gelu(pre, approximate=True).astype(jnp.bfloat16)
                return carry

            lax.fori_loop(0, rows // 64, body, 0)
            hidden_copy(j).start()

        rounds = max(planes, chunks)

        def up_step(m, carry):
            @pl.when(m < chunks)
            def _():
                for piece in range(1, pieces):
                    stages = stages_from(piece, up_bits)
                    if stages:
                        up_arrival(m, piece).wait_recv()
                        for stage in stages:
                            up_copy(m, piece, stage).start()

            @pl.when(m < planes)
            def _():
                pass_tokens(m)

            @pl.when(m < chunks)
            def _():
                for piece in range(1, pieces):
                    if not stages_from(piece, up_bits):
                        up_arrival(m, piece).wait_recv()
                w_local(m).wait()

            def sent(t, carry):
                distance = jnp.where(t // 2 < m, t // 2, m)
                j = jnp.where(t // 2 <= m, m, t // 2 - m - 1)
                block = jnp.where(t % 2 == 0, z - distance, z + distance)

                @pl.when((block >= 0) & (block < planes) & (j < chunks) & ((t % 2 == 0) | (distance > 0)))
                def _():
                    at = pl.ds(pl.multiple_of(block * shard, shard), shard)
                    ps[j, at, pl.ds(0, hj)] = dot(xp[at, :], wb[j]).astype(jnp.bfloat16)
                    partial_copy(j, block).start()
                return carry

            lax.fori_loop(0, 2 * (2 * m + 1), sent, 0)
            for q in early:
                @pl.when(m == EARLY_V[q])
                def _():
                    start_down(q)

            for j in range(2):
                @pl.when((m >= planes) & (2 * (m - planes) + j < chunks))
                def _():
                    finish(2 * (m - planes) + j)
            return carry

        lax.fori_loop(0, rounds, up_step, 0)
        for q in range(len(early), col_chunks):
            start_down(q)
        lax.fori_loop(0, col_chunks, start_down_core, 0)

        def finish_rest(j, carry):
            finish(j)
            return carry

        lax.fori_loop(min(2 * (rounds - planes), chunks), chunks, finish_rest, 0)
        shard_send.wait_send()

        def settle_up(j, carry):
            for piece in range(pieces):
                for stage in stages_from(piece, up_bits):
                    up_copy(j, piece, stage).wait_send()
            for block in range(planes):
                partial_copy(j, block).wait_send()
            return carry

        lax.fori_loop(0, chunks, settle_up, 0)
        small[2].wait()
        small[3].wait()

        part = rows // ROW_SPLIT
        items = col_chunks * ROW_SPLIT
        crossed = n_half * (slots - 1)
        entering = 2 * ((1 - n_half) * (slots - 1)) + 1 - n_half

        def rows_of(i):
            return pl.ds(pl.multiple_of((i % ROW_SPLIT) * part, part), part)

        def lanes_of(u):
            return pl.ds(pl.multiple_of(u * slot_width, slot_width), slot_width)

        def sums(i, u, other):
            return ps.at[i // ROW_SPLIT + col_chunks * other, rows_of(i), lanes_of(u)]

        def z_copy(i, lane, src, up):
            return pltpu.make_async_remote_copy(
                src_ref=src, dst_ref=(zu if up else zd).at[lane, i],
                send_sem=z_send.at[lane, i], recv_sem=(zu_recv if up else zd_recv).at[lane, i],
                device_id={"tp": z + 1 if up else z - 1}, device_id_type=MESH)

        def final_copy(i, u):
            return pltpu.make_async_remote_copy(
                src_ref=sums(i, u, 1), dst_ref=fr.at[i], send_sem=f_send.at[i], recv_sem=f_recv.at[i],
                device_id=near(n_bit), device_id_type=MESH)

        def cross_copy(i):
            return pltpu.make_async_remote_copy(
                src_ref=sums(i, crossed, 1), dst_ref=cr.at[i], send_sem=c_send.at[i], recv_sem=c_recv.at[i],
                device_id=near(n_bit), device_id_type=MESH)

        def deliver(i, value):
            at = rows_of(i)
            for c in range(per_plane):
                place = pl.ds(pl.multiple_of(c * out_block + (i // ROW_SPLIT) * cols, cols), cols)
                total = ob[at, place].astype(jnp.float32) + value[:, pl.ds(c * cols, cols)].astype(jnp.float32)
                ob[at, place] = (total + db[:, place]).astype(jnp.bfloat16)

        def depth_of(to):
            above = planes - 1 - z
            return jnp.where(z < to, z, jnp.where(z > to, above, jnp.where(z > above, z, above)))

        def lane_source(i, lane):
            if lane < slots:
                return sums(i, lane, 0), 2 * lane + n_half
            if lane < 2 * slots - 1:
                u = lane - slots + 1 - n_half
                return sums(i, u, 1), 2 * u + n_half
            return cr.at[i], entering

        def chain(s, lane):
            _, to = lane_source(0, lane)
            late = 1 if lane < slots else items + 1 if lane < 2 * slots - 1 else items + 2
            i = s - late - depth_of(to)

            @pl.when((i >= 0) & (i < items))
            def _():
                src, _ = lane_source(i, lane)
                if lane == 2 * slots - 1:
                    cross_copy(i).wait_recv()

                @pl.when((z > 0) & (z <= to))
                def _():
                    z_copy(i, lane, src, True).wait_recv()
                    src[...] = (src[...].astype(jnp.float32) + zu[lane, i].astype(jnp.float32)).astype(jnp.bfloat16)

                @pl.when((z < planes - 1) & (z >= to))
                def _():
                    z_copy(i, lane, src, False).wait_recv()
                    src[...] = (src[...].astype(jnp.float32) + zd[lane, i].astype(jnp.float32)).astype(jnp.bfloat16)

                @pl.when(z < to)
                def _():
                    z_copy(i, lane, src, True).start()

                @pl.when(z > to)
                def _():
                    z_copy(i, lane, src, False).start()

                @pl.when(z == to)
                def _():
                    if slots <= lane < 2 * slots - 1:
                        final_copy(i, lane - slots + 1 - n_half).start()
                    else:
                        deliver(i, src)

        def down_dot(src, i, other):
            q = i // ROW_SPLIT
            ps[q + col_chunks * other, rows_of(i), pl.ds(0, cols * pieces)] = dot(src[rows_of(i), :], vb[q]).astype(jnp.bfloat16)

        def down_step(s, carry):
            q = s // ROW_SPLIT
            fresh = (s < items) & (s % ROW_SPLIT == 0)

            @pl.when(fresh)
            def _():
                for piece in range(1, pieces):
                    stages = stages_from(piece, down_bits)
                    if stages:
                        down_arrival(q, piece).wait_recv()
                        for stage in stages:
                            down_copy(q, piece, stage).start()
                        v_local(q, piece).start()
                v_local(q, 0).start()

            for lane in range(2 * slots):
                chain(s, lane)

            @pl.when(fresh)
            def _():
                for piece in range(1, pieces):
                    if not stages_from(piece, down_bits):
                        down_arrival(q, piece).wait_recv()
                        v_local(q, piece).start()
                for piece in range(pieces):
                    v_local(q, piece).wait()

            @pl.when(s == items)
            def _():
                for j in range(chunks):
                    hidden_copy(j).wait_recv()

            @pl.when(s < items)
            def _():
                down_dot(hid, s, 0)

            @pl.when((s >= items) & (s < 2 * items))
            def _():
                down_dot(hx, s - items, 1)
                cross_copy(s - items).start()
            return carry

        lax.fori_loop(0, 2 * items + planes + 2, down_step, 0)

        @pl.when(z % 2 != n_half)
        def _():
            def body(i, carry):
                @pl.when(z != entering)
                def _():
                    final_copy(i, 0).wait_recv()
                    deliver(i, fr.at[i])
                return carry

            lax.fori_loop(0, items, body, 0)

        write = pltpu.make_async_copy(ob, out, misc_sem.at[0])
        write.start()

        def settle_down(q, carry):
            for piece in range(pieces):
                for stage in stages_from(piece, down_bits):
                    down_copy(q, piece, stage).wait_send()
            return carry

        lax.fori_loop(0, col_chunks, settle_down, 0)

        def settle_sums(i, carry):
            cross_copy(i).wait_send()
            for lane in range(2 * slots):
                src, to = lane_source(i, lane)

                @pl.when(z != to)
                def _():
                    z_copy(i, lane, src, True).wait_send()

                if slots <= lane < 2 * slots - 1:
                    @pl.when(z == to)
                    def _():
                        final_copy(i, lane - slots + 1 - n_half).wait_send()
            return carry

        lax.fori_loop(0, items, settle_sums, 0)

        def settle_hidden(j, carry):
            hidden_copy(j).wait_send()
            return carry

        lax.fori_loop(0, chunks, settle_hidden, 0)
        for distance in range(planes - 1):
            @pl.when((z >= distance) & (z < planes - 1))
            def _():
                pass_on(distance, True).wait_send()

            @pl.when((z + distance <= planes - 1) & (z > 0))
            def _():
                pass_on(distance, False).wait_send()
        write.wait()

    def per_device(tokens, norm_gain, up_weight, up_bias, down_weight, down_bias):
        rows, width = tokens.shape
        depth, hidden = up_weight.shape
        out_block = down_weight.shape[1]
        own_width = down_bias.shape[0]
        hj = chunk_of(hidden, HID_CHUNK)
        cols = chunk_of(out_block, COL_CHUNK)
        chunks, col_chunks = hidden // hj, out_block // cols
        half, shard = width // 2, rows // planes
        slab = cols * pieces
        items, part = col_chunks * ROW_SPLIT, rows // ROW_SPLIT
        bf, f32 = jnp.bfloat16, jnp.float32
        dma = pltpu.SemaphoreType.DMA
        shared = (chunks, half, hj) == (col_chunks, hidden, slab)
        scratch = [
            pltpu.VMEM((2, shard, width), bf),
            pltpu.VMEM((shard, half), bf),
            pltpu.VMEM((rows, half), bf),
            pltpu.VMEM((rows, half), bf),
            pltpu.VMEM((chunks, half, hj), bf),
            pltpu.VMEM((max(chunks, 2 * col_chunks), rows, max(hj, slab)), bf),
            pltpu.VMEM((chunks, rows, hj), bf),
            pltpu.VMEM((rows, hj), f32),
            pltpu.VMEM((rows, hidden), bf),
            pltpu.VMEM((rows, hidden), bf),
            pltpu.VMEM((2 * slots, items, part, per_plane * cols), bf),
            pltpu.VMEM((2 * slots, items, part, per_plane * cols), bf),
            pltpu.VMEM((items, part, per_plane * cols), bf),
            pltpu.VMEM((items, part, per_plane * cols), bf),
            pltpu.VMEM((rows, own_width), bf),
        ]
        if not shared:
            scratch.append(pltpu.VMEM((col_chunks, hidden, slab), bf))
        scratch += [
            pltpu.VMEM((1, width), bf),
            pltpu.VMEM((1, hidden), f32),
            pltpu.VMEM((1, own_width), f32),
            dma((2,)), dma((4,)), dma((chunks,)), dma((col_chunks, pieces)),
            dma((chunks, pieces - 1)), dma((chunks, pieces - 1)),
            dma((col_chunks, pieces - 1)), dma((col_chunks, pieces - 1)),
            dma, dma,
            dma((planes,)), dma((planes,)), dma((planes,)), dma((planes,)),
            dma((chunks, planes)), dma((chunks, planes)), dma((chunks,)), dma((chunks,)),
            dma((2 * slots, items)), dma((2 * slots, items)), dma((2 * slots, items)),
            dma((2, items)), dma((2, items)),
        ]
        hbm = pl.BlockSpec(memory_space=pltpu.HBM)
        result, _ = pl.pallas_call(
            kernel,
            out_shape=(
                jax.ShapeDtypeStruct((rows, own_width), bf),
                jax.ShapeDtypeStruct((col_chunks, hidden, slab), bf),
            ),
            in_specs=[hbm] * 6,
            out_specs=(hbm, hbm),
            scratch_shapes=scratch,
            compiler_params=pltpu.CompilerParams(
                collective_id=0, has_side_effects=True, vmem_limit_bytes=67043328),
        )(tokens, norm_gain[None, :], up_weight, up_bias[None, :], down_weight, down_bias[None, :])
        return result

    return per_device


def solution(mesh):
    in_specs = (P("grp", None), P(), P("grp", "tp"), P("tp"), P("tp", "grp"), P("tp"))
    return jax.shard_map(
        build(mesh.shape["grp"], mesh.shape["tp"]),
        mesh=mesh, in_specs=in_specs, out_specs=P("grp", "tp"), check_vma=False,
    )
```

```python
import functools

import jax
import jax.numpy as jnp
from jax import lax
from jax.experimental import pallas as pl
from jax.experimental.pallas import tpu as pltpu
from jax.sharding import PartitionSpec as P

MESH = pl.DeviceIdType.MESH
HID_CHUNK = 512
COL_CHUNK = 128
ROW_SPLIT = 2
EARLY_V = (-1, 1)


def chunk_of(extent, wanted):
    step = min(wanted, extent)
    while extent % step:
        step -= 128
    return step


def order_of(col_chunks, splits):
    own = [(0, q, h) for q in range(col_chunks) for h in range(splits)]
    last = col_chunks - 1
    other = [(1, q, 0) for q in range(last)]
    later = [(1, q, h) for h in range(1, splits) for q in range(col_chunks)]
    other += later[:3] + [(1, last, 0)] + later[3:]
    order, loaded, turn = [], -1, 0
    while own or other:
        ready = other and other[0][1] <= loaded and len(order) >= 2 * splits
        if own and (turn == 0 or not ready):
            order.append(own.pop(0))
            loaded, turn = order[-1][1], 1
        elif ready:
            order.append(other.pop(0))
            turn = 0
        if len(order) < 2 * splits:
            turn = 0
    return order


def dot(a, b):
    return jnp.dot(a, b, preferred_element_type=jnp.float32)


def build(groups, planes):
    bits = groups.bit_length() - 1
    k_bit, n_bit = bits - 1, 1
    up_bits = [b for b in range(1, bits) if b != k_bit] + [0]
    down_bits = [b for b in range(bits - 1, 0, -1) if b != n_bit] + [0]
    per_plane = groups // planes
    pieces = groups // 2
    slots = planes // 2

    def masks_of(order):
        masks = [()]
        for bit in order:
            masks = masks + [m + (bit,) for m in masks]
        return masks

    up_masks, down_masks = masks_of(up_bits), masks_of(down_bits)

    def stages_from(piece, order):
        return [s for s in range(len(order)) if (1 << s) > piece]

    def kernel(
        tok, gain, w, ubias, v, dbias, out, vh,
        tk, sh, xo, xp, wb, ps, pr, acc, hid, hx, zu, zd, fr, cr, ob, *rest,
    ):
        rest = list(rest)
        vb = rest.pop(0) if len(rest) == 27 else wb
        (gv, ub, db, tk_sem, misc_sem, wl_sem, vl_sem,
         up_send, up_recv, dn_send, dn_recv, x_send, x_recv,
         zxu_send, zxu_recv, zxd_send, zxd_recv,
         p_send, p_recv, h_send, h_recv, z_send, zu_recv, zd_recv, f_sem, c_sem) = rest
        f_send, f_recv, c_send, c_recv = f_sem.at[0], f_sem.at[1], c_sem.at[0], c_sem.at[1]

        me = lax.axis_index("grp")
        z = lax.axis_index("tp")
        rows, width = tok.shape
        depth, hidden = w.shape
        out_block = v.shape[1]
        own_width = out.shape[1]
        half = width // 2
        chunks, _, hj = wb.shape
        cols = vb.shape[2] // pieces
        col_chunks = vb.shape[0]
        slot_width = per_plane * cols
        shard = rows // planes

        def bit_of(b):
            return (me // (1 << b)) % 2

        def flipped(index_bits):
            index = me
            for b in index_bits:
                index = index + (1 - 2 * bit_of(b)) * (1 << b)
            return index

        def near(b):
            return {"grp": flipped((b,))}

        k_half, n_half = bit_of(k_bit), bit_of(n_bit)

        def up_place(mask):
            return pl.multiple_of((flipped(mask) % pieces) * depth, depth)

        def down_place(mask):
            block = flipped(mask)
            return pl.multiple_of(((block // 4) * 2 + block % 2) * cols, cols)

        def up_copy(j, piece, stage):
            place = pl.ds(up_place(up_masks[piece]), depth)
            landing = wb.at[j, place, :]
            source = w.at[:, pl.ds(pl.multiple_of(j * hj, hj), hj)] if piece == 0 else landing
            slot = piece + (1 << stage) - 1
            return pltpu.make_async_remote_copy(
                src_ref=source, dst_ref=landing,
                send_sem=up_send.at[j, slot], recv_sem=up_recv.at[j, slot],
                device_id=near(up_bits[stage]), device_id_type=MESH)

        def up_arrival(j, piece):
            place = pl.ds(up_place(up_masks[piece]), depth)
            landing = wb.at[j, place, :]
            stage = piece.bit_length() - 1
            return pltpu.make_async_remote_copy(
                src_ref=landing, dst_ref=landing,
                send_sem=up_send.at[j, piece - 1], recv_sem=up_recv.at[j, piece - 1],
                device_id=near(up_bits[stage]), device_id_type=MESH)

        def w_local(j):
            return pltpu.make_async_copy(
                w.at[:, pl.ds(pl.multiple_of(j * hj, hj), hj)],
                wb.at[j, pl.ds(up_place(()), depth), :], wl_sem.at[j])

        def down_copy(q, piece, stage):
            place = pl.ds(down_place(down_masks[piece]), cols)
            landing = vh.at[q, :, place]
            source = v.at[:, pl.ds(pl.multiple_of(q * cols, cols), cols)] if piece == 0 else landing
            slot = piece + (1 << stage) - 1
            return pltpu.make_async_remote_copy(
                src_ref=source, dst_ref=landing,
                send_sem=dn_send.at[q, slot], recv_sem=dn_recv.at[q, slot],
                device_id=near(down_bits[stage]), device_id_type=MESH)

        def down_arrival(q, piece):
            landing = vh.at[q, :, pl.ds(down_place(down_masks[piece]), cols)]
            stage = piece.bit_length() - 1
            return pltpu.make_async_remote_copy(
                src_ref=landing, dst_ref=landing,
                send_sem=dn_send.at[q, piece - 1], recv_sem=dn_recv.at[q, piece - 1],
                device_id=near(down_bits[stage]), device_id_type=MESH)

        def v_local(q, piece):
            place = pl.ds(down_place(down_masks[piece]), cols)
            source = v.at[:, pl.ds(pl.multiple_of(q * cols, cols), cols)] if piece == 0 else vh.at[q, :, place]
            return pltpu.make_async_copy(source, vb.at[q, :, place], vl_sem.at[q, piece])

        barrier = pltpu.get_barrier_semaphore()
        for b in range(bits):
            pl.semaphore_signal(barrier, inc=1, device_id=near(b), device_id_type=MESH)

        @pl.when(z > 0)
        def _():
            pl.semaphore_signal(barrier, inc=1, device_id={"tp": z - 1}, device_id_type=MESH)

        @pl.when(z < planes - 1)
        def _():
            pl.semaphore_signal(barrier, inc=1, device_id={"tp": z + 1}, device_id_type=MESH)

        shard_rows = pl.ds(pl.multiple_of(z * shard, shard), shard)

        def token_copy(index, slot):
            source = shard_rows if index < 0 else pl.ds(index * shard, shard)
            return pltpu.make_async_copy(tok.at[source, :], tk.at[slot], tk_sem.at[slot])

        token_copy(-1, 0).start()
        token_copy(0, 1).start()
        small = [
            pltpu.make_async_copy(gain, gv, misc_sem.at[0]),
            pltpu.make_async_copy(ubias, ub, misc_sem.at[1]),
            pltpu.make_async_copy(dbias, db, misc_sem.at[2]),
            pltpu.make_async_copy(
                tok.at[:, pl.ds(pl.multiple_of(z * own_width, own_width), own_width)], ob, misc_sem.at[3]),
        ]
        for copy in small:
            copy.start()

        neighbours = bits + jnp.where(z > 0, 1, 0) + jnp.where(z < planes - 1, 1, 0)
        pl.semaphore_wait(barrier, neighbours)

        def start_up(j, carry):
            for stage in range(len(up_bits)):
                up_copy(j, 0, stage).start()
            w_local(j).start()
            return carry

        lax.fori_loop(0, chunks, start_up, 0)
        small[0].wait()

        tile = 16

        def normalise(slot, column, dst, base):
            def body(i, carry):
                at = pl.multiple_of(i * tile, tile)
                values = tk[slot, pl.ds(at, tile), :].astype(jnp.float32)
                centre = jnp.mean(values, axis=1, keepdims=True)
                shifted = values - centre
                scale = lax.rsqrt(jnp.mean(shifted * shifted, axis=1, keepdims=True) + 1e-06)
                part = tk[slot, pl.ds(at, tile), pl.ds(column, half)].astype(jnp.float32)
                normed = (part - centre) * scale * gv[:, pl.ds(column, half)].astype(jnp.float32)
                dst[pl.ds(pl.multiple_of(base + at, tile), tile), :] = normed.astype(jnp.bfloat16)
                return carry

            lax.fori_loop(0, shard // tile, body, 0)

        own_column = pl.multiple_of(k_half * half, half)
        other_column = pl.multiple_of((1 - k_half) * half, half)

        token_copy(-1, 0).wait()
        normalise(0, other_column, sh, 0)
        shard_send = pltpu.make_async_remote_copy(
            src_ref=sh, dst_ref=xp.at[shard_rows, :],
            send_sem=x_send, recv_sem=x_recv, device_id=near(k_bit), device_id_type=MESH)
        shard_send.start()

        def start_down(q):
            down_copy(q, 0, 0).start()

        early = [q for q in range(len(EARLY_V)) if q < col_chunks]
        for q in early:
            if EARLY_V[q] < 0:
                start_down(q)

        def start_down_core(q, carry):
            for stage in range(1, len(down_bits)):
                down_copy(q, 0, stage).start()
            return carry

        for c in range(planes):
            slot = (c + 1) % 2
            if c + 1 < planes:
                token_copy(c + 1, 1 - slot).start()
            token_copy(c, slot).wait()
            normalise(slot, own_column, xo, c * shard)

        def pass_on(distance, rising):
            source = z - distance if rising else z + distance
            place = pl.ds(pl.multiple_of(source * shard, shard), shard)
            return pltpu.make_async_remote_copy(
                src_ref=xp.at[place, :], dst_ref=xp.at[place, :],
                send_sem=(zxu_send if rising else zxd_send).at[distance],
                recv_sem=(zxu_recv if rising else zxd_recv).at[distance],
                device_id={"tp": z + 1 if rising else z - 1}, device_id_type=MESH)

        def arrival(distance, rising):
            source = z - distance if rising else z + distance
            place = pl.ds(pl.multiple_of(source * shard, shard), shard)
            return pltpu.make_async_remote_copy(
                src_ref=xp.at[place, :], dst_ref=xp.at[place, :],
                send_sem=(zxu_send if rising else zxd_send).at[distance - 1],
                recv_sem=(zxu_recv if rising else zxd_recv).at[distance - 1],
                device_id={"tp": z - 1 if rising else z + 1}, device_id_type=MESH)

        def pass_tokens(distance):
            @pl.when(distance == 0)
            def _():
                shard_send.wait_recv()

            @pl.when((distance > 0) & (z >= distance))
            def _():
                arrival(distance, True).wait_recv()

            @pl.when((distance > 0) & (z + distance <= planes - 1))
            def _():
                arrival(distance, False).wait_recv()

            @pl.when((z >= distance) & (z < planes - 1) & (distance < planes - 1))
            def _():
                pass_on(distance, True).start()

            @pl.when((z + distance <= planes - 1) & (z > 0) & (distance < planes - 1))
            def _():
                pass_on(distance, False).start()

        small[1].wait()

        def partial_copy(j, block):
            place = pl.ds(pl.multiple_of(block * shard, shard), shard)
            return pltpu.make_async_remote_copy(
                src_ref=ps.at[j, place, pl.ds(0, hj)], dst_ref=pr.at[j, place, :],
                send_sem=p_send.at[j, block], recv_sem=p_recv.at[j, block],
                device_id=near(k_bit), device_id_type=MESH)

        part = rows // ROW_SPLIT
        items = col_chunks * ROW_SPLIT

        def rows_of(i):
            return pl.ds(pl.multiple_of((i % ROW_SPLIT) * part, part), part)

        def hidden_copy(j, h):
            place = pl.ds(pl.multiple_of(j * hj, hj), hj)
            return pltpu.make_async_remote_copy(
                src_ref=hid.at[rows_of(h), place], dst_ref=hx.at[rows_of(h), place],
                send_sem=h_send.at[j, h], recv_sem=h_recv.at[j, h],
                device_id=near(n_bit), device_id_type=MESH)

        row_tile = min(256, rows)

        def finish(j):
            place = pl.ds(pl.multiple_of(j * hj, hj), hj)

            def kept(i, carry):
                at = pl.ds(pl.multiple_of(i * row_tile, row_tile), row_tile)
                acc[at, :] = dot(xo[at, :], wb[j])
                return carry

            lax.fori_loop(0, rows // row_tile, kept, 0)
            for block in range(planes):
                partial_copy(j, block).wait_recv()

            def body(i, carry):
                at = pl.ds(pl.multiple_of(i * 64, 64), 64)
                pre = acc[at, :] + pr[j, at, :].astype(jnp.float32) + ub[:, place]
                hid[at, place] = jax.nn.gelu(pre, approximate=True).astype(jnp.bfloat16)
                return carry

            lax.fori_loop(0, rows // 64, body, 0)
            hidden_copy(j, 0).start()

        rounds = max(planes, chunks)

        def up_step(m, carry):
            @pl.when(m < chunks)
            def _():
                for piece in range(1, pieces):
                    stages = stages_from(piece, up_bits)
                    if stages:
                        up_arrival(m, piece).wait_recv()
                        for stage in stages:
                            up_copy(m, piece, stage).start()

            @pl.when(m < planes)
            def _():
                pass_tokens(m)

            @pl.when(m < chunks)
            def _():
                for piece in range(1, pieces):
                    if not stages_from(piece, up_bits):
                        up_arrival(m, piece).wait_recv()
                w_local(m).wait()

            def sent(t, carry):
                distance = jnp.where(t // 2 < m, t // 2, m)
                j = jnp.where(t // 2 <= m, m, t // 2 - m - 1)
                block = jnp.where(t % 2 == 0, z - distance, z + distance)

                @pl.when((block >= 0) & (block < planes) & (j < chunks) & ((t % 2 == 0) | (distance > 0)))
                def _():
                    at = pl.ds(pl.multiple_of(block * shard, shard), shard)
                    ps[j, at, pl.ds(0, hj)] = dot(xp[at, :], wb[j]).astype(jnp.bfloat16)
                    partial_copy(j, block).start()
                return carry

            lax.fori_loop(0, 2 * (2 * m + 1), sent, 0)
            for q in early:
                @pl.when(m == EARLY_V[q])
                def _():
                    start_down(q)

            for j in range(2):
                @pl.when((m >= planes) & (2 * (m - planes) + j < chunks))
                def _():
                    finish(2 * (m - planes) + j)
            return carry

        lax.fori_loop(0, rounds, up_step, 0)
        for q in range(len(early), col_chunks):
            start_down(q)
        lax.fori_loop(0, col_chunks, start_down_core, 0)

        def finish_rest(j, carry):
            finish(j)
            return carry

        lax.fori_loop(min(2 * (rounds - planes), chunks), chunks, finish_rest, 0)
        shard_send.wait_send()

        def settle_up(j, carry):
            for piece in range(pieces):
                for stage in stages_from(piece, up_bits):
                    up_copy(j, piece, stage).wait_send()
            for block in range(planes):
                partial_copy(j, block).wait_send()
            return carry

        lax.fori_loop(0, chunks, settle_up, 0)
        small[2].wait()
        small[3].wait()

        crossed = n_half * (slots - 1)
        entering = 2 * ((1 - n_half) * (slots - 1)) + 1 - n_half
        order = order_of(col_chunks, ROW_SPLIT)
        first_other = [k for k in range(len(order)) if order[k][0]][0]
        late_hidden = [(j, h) for h in range(1, ROW_SPLIT) for j in range(chunks)]

        def code_of(s):
            code = -1
            for k in range(len(order)):
                kind, q, h = order[k]
                code = jnp.where(s == k, kind * items + q * ROW_SPLIT + h, code)
            return code

        def lanes_of(u):
            return pl.ds(pl.multiple_of(u * slot_width, slot_width), slot_width)

        def sums(i, u, other):
            return ps.at[i // ROW_SPLIT + col_chunks * other, rows_of(i), lanes_of(u)]

        def z_copy(i, lane, src, up):
            return pltpu.make_async_remote_copy(
                src_ref=src, dst_ref=(zu if up else zd).at[lane, i],
                send_sem=z_send.at[lane, i], recv_sem=(zu_recv if up else zd_recv).at[lane, i],
                device_id={"tp": z + 1 if up else z - 1}, device_id_type=MESH)

        def final_copy(i, u):
            return pltpu.make_async_remote_copy(
                src_ref=sums(i, u, 1), dst_ref=fr.at[i], send_sem=f_send.at[i], recv_sem=f_recv.at[i],
                device_id=near(n_bit), device_id_type=MESH)

        def cross_copy(i):
            return pltpu.make_async_remote_copy(
                src_ref=sums(i, crossed, 1), dst_ref=cr.at[i], send_sem=c_send.at[i], recv_sem=c_recv.at[i],
                device_id=near(n_bit), device_id_type=MESH)

        def deliver(i, value):
            at = rows_of(i)
            for c in range(per_plane):
                place = pl.ds(pl.multiple_of(c * out_block + (i // ROW_SPLIT) * cols, cols), cols)
                total = ob[at, place].astype(jnp.float32) + value[:, pl.ds(c * cols, cols)].astype(jnp.float32)
                ob[at, place] = (total + db[:, place]).astype(jnp.bfloat16)

        def depth_of(to):
            above = planes - 1 - z
            return jnp.where(z < to, z, jnp.where(z > to, above, jnp.where(z > above, z, above)))

        def lane_source(i, lane):
            if lane < slots:
                return sums(i, lane, 0), 2 * lane + n_half
            if lane < 2 * slots - 1:
                u = lane - slots + 1 - n_half
                return sums(i, u, 1), 2 * u + n_half
            return cr.at[i], entering

        def chain(s, lane):
            _, to = lane_source(0, lane)
            late = 2 if lane == 2 * slots - 1 else 1
            code = code_of(s - late - depth_of(to))
            i = code if lane < slots else code - items

            @pl.when((i >= 0) & (i < items))
            def _():
                src, _ = lane_source(i, lane)
                if lane == 2 * slots - 1:
                    cross_copy(i).wait_recv()

                @pl.when((z > 0) & (z <= to))
                def _():
                    z_copy(i, lane, src, True).wait_recv()
                    src[...] = (src[...].astype(jnp.float32) + zu[lane, i].astype(jnp.float32)).astype(jnp.bfloat16)

                @pl.when((z < planes - 1) & (z >= to))
                def _():
                    z_copy(i, lane, src, False).wait_recv()
                    src[...] = (src[...].astype(jnp.float32) + zd[lane, i].astype(jnp.float32)).astype(jnp.bfloat16)

                @pl.when(z < to)
                def _():
                    z_copy(i, lane, src, True).start()

                @pl.when(z > to)
                def _():
                    z_copy(i, lane, src, False).start()

                @pl.when(z == to)
                def _():
                    if slots <= lane < 2 * slots - 1:
                        final_copy(i, lane - slots + 1 - n_half).start()
                    else:
                        deliver(i, src)

        def down_dot(src, i, other):
            q = i // ROW_SPLIT
            ps[q + col_chunks * other, rows_of(i), pl.ds(0, cols * pieces)] = dot(src[rows_of(i), :], vb[q]).astype(jnp.bfloat16)

        def down_step(s, carry):
            code = code_of(s)
            i = code % items
            q = i // ROW_SPLIT
            own, other = (code >= 0) & (code < items), code >= items
            fresh = own & (i % ROW_SPLIT == 0)

            @pl.when(fresh)
            def _():
                for piece in range(1, pieces):
                    stages = stages_from(piece, down_bits)
                    if stages:
                        down_arrival(q, piece).wait_recv()
                        for stage in stages:
                            down_copy(q, piece, stage).start()
                        v_local(q, piece).start()
                v_local(q, 0).start()

            for lane in range(2 * slots):
                chain(s, lane)

            @pl.when(fresh)
            def _():
                for piece in range(1, pieces):
                    if not stages_from(piece, down_bits):
                        down_arrival(q, piece).wait_recv()
                        v_local(q, piece).start()
                for piece in range(pieces):
                    v_local(q, piece).wait()

            for k in range(len(late_hidden)):
                @pl.when(s == first_other + k + (k + 1) // 2)
                def _():
                    hidden_copy(*late_hidden[k]).start()

            @pl.when(other & (q == 0))
            def _():
                for j in range(chunks):
                    hidden_copy(j, i % ROW_SPLIT).wait_recv()

            @pl.when(own)
            def _():
                down_dot(hid, i, 0)

            @pl.when(other)
            def _():
                down_dot(hx, i, 1)
                cross_copy(i).start()
            return carry

        lax.fori_loop(0, 2 * items + planes + 2, down_step, 0)

        @pl.when(z % 2 != n_half)
        def _():
            def body(i, carry):
                @pl.when(z != entering)
                def _():
                    final_copy(i, 0).wait_recv()
                    deliver(i, fr.at[i])
                return carry

            lax.fori_loop(0, items, body, 0)

        write = pltpu.make_async_copy(ob, out, misc_sem.at[0])
        write.start()

        def settle_down(q, carry):
            for piece in range(pieces):
                for stage in stages_from(piece, down_bits):
                    down_copy(q, piece, stage).wait_send()
            return carry

        lax.fori_loop(0, col_chunks, settle_down, 0)

        def settle_sums(i, carry):
            cross_copy(i).wait_send()
            for lane in range(2 * slots):
                src, to = lane_source(i, lane)

                @pl.when(z != to)
                def _():
                    z_copy(i, lane, src, True).wait_send()

                if slots <= lane < 2 * slots - 1:
                    @pl.when(z == to)
                    def _():
                        final_copy(i, lane - slots + 1 - n_half).wait_send()
            return carry

        lax.fori_loop(0, items, settle_sums, 0)

        def settle_hidden(j, carry):
            for h in range(ROW_SPLIT):
                hidden_copy(j, h).wait_send()
            return carry

        lax.fori_loop(0, chunks, settle_hidden, 0)
        for distance in range(planes - 1):
            @pl.when((z >= distance) & (z < planes - 1))
            def _():
                pass_on(distance, True).wait_send()

            @pl.when((z + distance <= planes - 1) & (z > 0))
            def _():
                pass_on(distance, False).wait_send()
        write.wait()

    def per_device(tokens, norm_gain, up_weight, up_bias, down_weight, down_bias):
        rows, width = tokens.shape
        depth, hidden = up_weight.shape
        out_block = down_weight.shape[1]
        own_width = down_bias.shape[0]
        hj = chunk_of(hidden, HID_CHUNK)
        cols = chunk_of(out_block, COL_CHUNK)
        chunks, col_chunks = hidden // hj, out_block // cols
        half, shard = width // 2, rows // planes
        slab = cols * pieces
        items, part = col_chunks * ROW_SPLIT, rows // ROW_SPLIT
        bf, f32 = jnp.bfloat16, jnp.float32
        dma = pltpu.SemaphoreType.DMA
        shared = (chunks, half, hj) == (col_chunks, hidden, slab)
        scratch = [
            pltpu.VMEM((2, shard, width), bf),
            pltpu.VMEM((shard, half), bf),
            pltpu.VMEM((rows, half), bf),
            pltpu.VMEM((rows, half), bf),
            pltpu.VMEM((chunks, half, hj), bf),
            pltpu.VMEM((max(chunks, 2 * col_chunks), rows, max(hj, slab)), bf),
            pltpu.VMEM((chunks, rows, hj), bf),
            pltpu.VMEM((rows, hj), f32),
            pltpu.VMEM((rows, hidden), bf),
            pltpu.VMEM((rows, hidden), bf),
            pltpu.VMEM((2 * slots, items, part, per_plane * cols), bf),
            pltpu.VMEM((2 * slots, items, part, per_plane * cols), bf),
            pltpu.VMEM((items, part, per_plane * cols), bf),
            pltpu.VMEM((items, part, per_plane * cols), bf),
            pltpu.VMEM((rows, own_width), bf),
        ]
        if not shared:
            scratch.append(pltpu.VMEM((col_chunks, hidden, slab), bf))
        scratch += [
            pltpu.VMEM((1, width), bf),
            pltpu.VMEM((1, hidden), f32),
            pltpu.VMEM((1, own_width), f32),
            dma((2,)), dma((4,)), dma((chunks,)), dma((col_chunks, pieces)),
            dma((chunks, pieces - 1)), dma((chunks, pieces - 1)),
            dma((col_chunks, pieces - 1)), dma((col_chunks, pieces - 1)),
            dma, dma,
            dma((planes,)), dma((planes,)), dma((planes,)), dma((planes,)),
            dma((chunks, planes)), dma((chunks, planes)), dma((chunks, ROW_SPLIT)), dma((chunks, ROW_SPLIT)),
            dma((2 * slots, items)), dma((2 * slots, items)), dma((2 * slots, items)),
            dma((2, items)), dma((2, items)),
        ]
        hbm = pl.BlockSpec(memory_space=pltpu.HBM)
        result, _ = pl.pallas_call(
            kernel,
            out_shape=(
                jax.ShapeDtypeStruct((rows, own_width), bf),
                jax.ShapeDtypeStruct((col_chunks, hidden, slab), bf),
            ),
            in_specs=[hbm] * 6,
            out_specs=(hbm, hbm),
            scratch_shapes=scratch,
            compiler_params=pltpu.CompilerParams(
                collective_id=0, has_side_effects=True, vmem_limit_bytes=67043328),
        )(tokens, norm_gain[None, :], up_weight, up_bias[None, :], down_weight, down_bias[None, :])
        return result

    return per_device


def solution(mesh):
    in_specs = (P("grp", None), P(), P("grp", "tp"), P("tp"), P("tp", "grp"), P("tp"))
    return jax.shard_map(
        build(mesh.shape["grp"], mesh.shape["tp"]),
        mesh=mesh, in_specs=in_specs, out_specs=P("grp", "tp"), check_vma=False,
    )
```

```python
import functools

import jax
import jax.numpy as jnp
from jax import lax
from jax.experimental import pallas as pl
from jax.experimental.pallas import tpu as pltpu
from jax.sharding import PartitionSpec as P

MESH = pl.DeviceIdType.MESH
HID_CHUNK = 512
COL_CHUNK = 128
ROW_SPLIT = 2
HOP_STEPS = 2
CROSS_STEPS = 2
FIRST_HIDDEN = 1
EARLY_V = (-1, 1)


def chunk_of(extent, wanted):
    step = min(wanted, extent)
    while extent % step:
        step -= 128
    return step


def order_of(col_chunks, splits, chunks):
    def columns_at(q):
        return 0 if q < 2 else int(splits * (3.25 + 2 * (q - 2)))

    def hidden_at(h):
        return 2 + 2 * chunks * h if h else FIRST_HIDDEN * splits

    own = [(0, q, h) for h in range(splits) for q in range(min(2, col_chunks))]
    own += [(0, q, h) for q in range(2, col_chunks) for h in range(splits)]
    other = [(1, q, h) for q in range(col_chunks) for h in range(splits)]
    other.sort(key=lambda item: (max(columns_at(item[1]), hidden_at(item[2])), item[2], item[1]))
    order, loaded, load = [], set(), [0, 0]
    while own or other:
        here = len(order)
        known = [item for item in other if item[1] in loaded]
        ready = [item for item in known if max(columns_at(item[1]), hidden_at(item[2])) <= here]
        own_ready = own and columns_at(own[0][1]) <= here
        if own and (own_ready and (not ready or load[0] <= load[1]) or not (own_ready or ready)):
            pick = own.pop(0)
            loaded.add(pick[1])
        else:
            pick = (ready or known)[0]
            other.remove(pick)
        load[pick[0]] += 2
        load[1 - pick[0]] += 1
        order.append(pick)
    return order


def dot(a, b):
    return jnp.dot(a, b, preferred_element_type=jnp.float32)


def build(groups, planes):
    bits = groups.bit_length() - 1
    k_bit, n_bit = bits - 1, 1
    up_bits = [b for b in range(1, bits) if b != k_bit] + [0]
    down_bits = [b for b in range(bits - 1, 0, -1) if b != n_bit] + [0]
    per_plane = groups // planes
    pieces = groups // 2
    slots = planes // 2

    def masks_of(order):
        masks = [()]
        for bit in order:
            masks = masks + [m + (bit,) for m in masks]
        return masks

    up_masks, down_masks = masks_of(up_bits), masks_of(down_bits)

    def stages_from(piece, order):
        return [s for s in range(len(order)) if (1 << s) > piece]

    def kernel(
        tok, gain, w, ubias, v, dbias, out, vh,
        tk, sh, xo, xp, wb, ps, pr, acc, hid, hx, zu, zd, fr, cr, ob, *rest,
    ):
        rest = list(rest)
        vb = rest.pop(0) if len(rest) == 29 else wb
        (gv, ub, db, gain_row, bias_row, tk_sem, misc_sem, wl_sem, vl_sem,
         up_send, up_recv, dn_send, dn_recv, x_send, x_recv,
         zxu_send, zxu_recv, zxd_send, zxd_recv,
         p_send, p_recv, h_send, h_recv, z_send, zu_recv, zd_recv, f_sem, c_sem) = rest
        f_send, f_recv, c_send, c_recv = f_sem.at[0], f_sem.at[1], c_sem.at[0], c_sem.at[1]

        me = lax.axis_index("grp")
        z = lax.axis_index("tp")
        rows, width = tok.shape
        depth, hidden = w.shape
        out_block = v.shape[1]
        own_width = out.shape[1]
        half = width // 2
        chunks, _, hj = wb.shape
        cols = vb.shape[2] // pieces
        col_chunks = vb.shape[0]
        slot_width = per_plane * cols
        shard = rows // planes

        def bit_of(b):
            return (me // (1 << b)) % 2

        def flipped(index_bits):
            index = me
            for b in index_bits:
                index = index + (1 - 2 * bit_of(b)) * (1 << b)
            return index

        def near(b):
            return {"grp": flipped((b,))}

        k_half, n_half = bit_of(k_bit), bit_of(n_bit)

        def up_place(mask):
            return pl.multiple_of((flipped(mask) % pieces) * depth, depth)

        def down_place(mask):
            block = flipped(mask)
            return pl.multiple_of(((block // 4) * 2 + block % 2) * cols, cols)

        def up_copy(j, piece, stage):
            place = pl.ds(up_place(up_masks[piece]), depth)
            landing = wb.at[j, place, :]
            source = w.at[:, pl.ds(pl.multiple_of(j * hj, hj), hj)] if piece == 0 else landing
            slot = piece + (1 << stage) - 1
            return pltpu.make_async_remote_copy(
                src_ref=source, dst_ref=landing,
                send_sem=up_send.at[j, slot], recv_sem=up_recv.at[j, slot],
                device_id=near(up_bits[stage]), device_id_type=MESH)

        def up_arrival(j, piece):
            place = pl.ds(up_place(up_masks[piece]), depth)
            landing = wb.at[j, place, :]
            stage = piece.bit_length() - 1
            return pltpu.make_async_remote_copy(
                src_ref=landing, dst_ref=landing,
                send_sem=up_send.at[j, piece - 1], recv_sem=up_recv.at[j, piece - 1],
                device_id=near(up_bits[stage]), device_id_type=MESH)

        def w_local(j):
            return pltpu.make_async_copy(
                w.at[:, pl.ds(pl.multiple_of(j * hj, hj), hj)],
                wb.at[j, pl.ds(up_place(()), depth), :], wl_sem.at[j])

        def down_copy(q, piece, stage):
            place = pl.ds(down_place(down_masks[piece]), cols)
            landing = vh.at[q, :, place]
            source = v.at[:, pl.ds(pl.multiple_of(q * cols, cols), cols)] if piece == 0 else landing
            slot = piece + (1 << stage) - 1
            return pltpu.make_async_remote_copy(
                src_ref=source, dst_ref=landing,
                send_sem=dn_send.at[q, slot], recv_sem=dn_recv.at[q, slot],
                device_id=near(down_bits[stage]), device_id_type=MESH)

        def down_arrival(q, piece):
            landing = vh.at[q, :, pl.ds(down_place(down_masks[piece]), cols)]
            stage = piece.bit_length() - 1
            return pltpu.make_async_remote_copy(
                src_ref=landing, dst_ref=landing,
                send_sem=dn_send.at[q, piece - 1], recv_sem=dn_recv.at[q, piece - 1],
                device_id=near(down_bits[stage]), device_id_type=MESH)

        def v_local(q, piece):
            place = pl.ds(down_place(down_masks[piece]), cols)
            source = v.at[:, pl.ds(pl.multiple_of(q * cols, cols), cols)] if piece == 0 else vh.at[q, :, place]
            return pltpu.make_async_copy(source, vb.at[q, :, place], vl_sem.at[q, piece])

        barrier = pltpu.get_barrier_semaphore()
        for b in range(bits):
            pl.semaphore_signal(barrier, inc=1, device_id=near(b), device_id_type=MESH)

        @pl.when(z > 0)
        def _():
            pl.semaphore_signal(barrier, inc=1, device_id={"tp": z - 1}, device_id_type=MESH)

        @pl.when(z < planes - 1)
        def _():
            pl.semaphore_signal(barrier, inc=1, device_id={"tp": z + 1}, device_id_type=MESH)

        shard_rows = pl.ds(pl.multiple_of(z * shard, shard), shard)

        def token_copy(index, slot):
            source = shard_rows if index < 0 else pl.ds(index * shard, shard)
            return pltpu.make_async_copy(tok.at[source, :], tk.at[slot], tk_sem.at[slot])

        token_copy(-1, 0).start()
        token_copy(0, 1).start()
        small = [
            pltpu.make_async_copy(gain, gain_row, misc_sem.at[0]),
            pltpu.make_async_copy(ubias, ub, misc_sem.at[1]),
            pltpu.make_async_copy(dbias, bias_row, misc_sem.at[2]),
            pltpu.make_async_copy(
                tok.at[:, pl.ds(pl.multiple_of(z * own_width, own_width), own_width)], ob, misc_sem.at[3]),
        ]
        for copy in small:
            copy.start()

        neighbours = bits + jnp.where(z > 0, 1, 0) + jnp.where(z < planes - 1, 1, 0)
        pl.semaphore_wait(barrier, neighbours)

        def start_up(j, carry):
            for stage in range(len(up_bits)):
                up_copy(j, 0, stage).start()
            w_local(j).start()
            return carry

        lax.fori_loop(0, chunks, start_up, 0)
        small[0].wait()
        gv[...] = gain_row[...].reshape(1, width)

        tile = 16

        def normalise(slot, column, dst, base):
            def body(i, carry):
                at = pl.multiple_of(i * tile, tile)
                values = tk[slot, pl.ds(at, tile), :].astype(jnp.float32)
                centre = jnp.mean(values, axis=1, keepdims=True)
                shifted = values - centre
                scale = lax.rsqrt(jnp.mean(shifted * shifted, axis=1, keepdims=True) + 1e-06)
                part = tk[slot, pl.ds(at, tile), pl.ds(column, half)].astype(jnp.float32)
                normed = (part - centre) * scale * gv[:, pl.ds(column, half)].astype(jnp.float32)
                dst[pl.ds(pl.multiple_of(base + at, tile), tile), :] = normed.astype(jnp.bfloat16)
                return carry

            lax.fori_loop(0, shard // tile, body, 0)

        own_column = pl.multiple_of(k_half * half, half)
        other_column = pl.multiple_of((1 - k_half) * half, half)

        token_copy(-1, 0).wait()
        normalise(0, other_column, sh, 0)
        shard_send = pltpu.make_async_remote_copy(
            src_ref=sh, dst_ref=xp.at[shard_rows, :],
            send_sem=x_send, recv_sem=x_recv, device_id=near(k_bit), device_id_type=MESH)
        shard_send.start()

        def start_down(q):
            down_copy(q, 0, 0).start()

        early = [q for q in range(len(EARLY_V)) if q < col_chunks]
        for q in early:
            if EARLY_V[q] < 0:
                start_down(q)

        def start_down_core(q, carry):
            for stage in range(1, len(down_bits)):
                down_copy(q, 0, stage).start()
            return carry

        for c in range(planes):
            slot = (c + 1) % 2
            if c + 1 < planes:
                token_copy(c + 1, 1 - slot).start()
            token_copy(c, slot).wait()
            normalise(slot, own_column, xo, c * shard)

        def pass_on(distance, rising):
            source = z - distance if rising else z + distance
            place = pl.ds(pl.multiple_of(source * shard, shard), shard)
            return pltpu.make_async_remote_copy(
                src_ref=xp.at[place, :], dst_ref=xp.at[place, :],
                send_sem=(zxu_send if rising else zxd_send).at[distance],
                recv_sem=(zxu_recv if rising else zxd_recv).at[distance],
                device_id={"tp": z + 1 if rising else z - 1}, device_id_type=MESH)

        def arrival(distance, rising):
            source = z - distance if rising else z + distance
            place = pl.ds(pl.multiple_of(source * shard, shard), shard)
            return pltpu.make_async_remote_copy(
                src_ref=xp.at[place, :], dst_ref=xp.at[place, :],
                send_sem=(zxu_send if rising else zxd_send).at[distance - 1],
                recv_sem=(zxu_recv if rising else zxd_recv).at[distance - 1],
                device_id={"tp": z - 1 if rising else z + 1}, device_id_type=MESH)

        def pass_tokens(distance):
            @pl.when(distance == 0)
            def _():
                shard_send.wait_recv()

            @pl.when((distance > 0) & (z >= distance))
            def _():
                arrival(distance, True).wait_recv()

            @pl.when((distance > 0) & (z + distance <= planes - 1))
            def _():
                arrival(distance, False).wait_recv()

            @pl.when((z >= distance) & (z < planes - 1) & (distance < planes - 1))
            def _():
                pass_on(distance, True).start()

            @pl.when((z + distance <= planes - 1) & (z > 0) & (distance < planes - 1))
            def _():
                pass_on(distance, False).start()

        small[1].wait()

        parked = ps.shape[0] - chunks

        def partial_copy(j, block):
            place = pl.ds(pl.multiple_of(block * shard, shard), shard)
            return pltpu.make_async_remote_copy(
                src_ref=ps.at[parked + j, place, pl.ds(0, hj)], dst_ref=pr.at[j, place, :],
                send_sem=p_send.at[j, block], recv_sem=p_recv.at[j, block],
                device_id=near(k_bit), device_id_type=MESH)

        part = rows // ROW_SPLIT
        items = col_chunks * ROW_SPLIT

        def rows_of(i):
            return pl.ds(pl.multiple_of((i % ROW_SPLIT) * part, part), part)

        def hidden_copy(j, h):
            place = pl.ds(pl.multiple_of(j * hj, hj), hj)
            return pltpu.make_async_remote_copy(
                src_ref=hid.at[rows_of(h), place], dst_ref=hx.at[rows_of(h), place],
                send_sem=h_send.at[j, h], recv_sem=h_recv.at[j, h],
                device_id=near(n_bit), device_id_type=MESH)

        row_tile = min(256, rows)

        def finish(j, h):
            place = pl.ds(pl.multiple_of(j * hj, hj), hj)
            acc[...] = dot(xo[rows_of(h), :], wb[j])
            for block in range(planes // ROW_SPLIT):
                partial_copy(j, h * (planes // ROW_SPLIT) + block).wait_recv()
            pre = acc[...] + pr[j, rows_of(h), :].astype(jnp.float32) + ub[:, place]
            hid[rows_of(h), place] = jax.nn.gelu(pre, approximate=True).astype(jnp.bfloat16)

            @pl.when(h == 0)
            def _():
                hidden_copy(j, 0).start()

        def finish_rows(j, first, last):
            def body(h, carry):
                finish(j, h)
                return carry

            lax.fori_loop(first, last, body, 0)

        rounds = max(planes, chunks)

        def up_step(m, carry):
            for j in range(2):
                @pl.when((m >= planes) & (2 * (m - planes) + j < chunks - 1))
                def _():
                    finish_rows(2 * (m - planes) + j, 0, ROW_SPLIT)

            @pl.when(m < chunks)
            def _():
                for piece in range(1, pieces):
                    stages = stages_from(piece, up_bits)
                    if stages:
                        up_arrival(m, piece).wait_recv()
                        for stage in stages:
                            up_copy(m, piece, stage).start()

            @pl.when(m < planes)
            def _():
                pass_tokens(m)

            @pl.when(m < chunks)
            def _():
                for piece in range(1, pieces):
                    if not stages_from(piece, up_bits):
                        up_arrival(m, piece).wait_recv()
                w_local(m).wait()

            def sent(t, carry):
                distance = jnp.where(t // 2 < m, t // 2, m)
                j = jnp.where(t // 2 <= m, m, t // 2 - m - 1)
                block = jnp.where(t % 2 == 0, z - distance, z + distance)
                straight = m >= planes
                block = jnp.where(straight, t, block)
                j = jnp.where(straight, m, j)

                @pl.when((block >= 0) & (block < planes) & (j < chunks) & (straight | (t % 2 == 0) | (distance > 0)))
                def _():
                    at = pl.ds(pl.multiple_of(block * shard, shard), shard)
                    ps[parked + j, at, pl.ds(0, hj)] = dot(xp[at, :], wb[j]).astype(jnp.bfloat16)
                    partial_copy(j, block).start()
                return carry

            lax.fori_loop(0, 2 * (2 * m + 1), sent, 0)
            for q in early:
                @pl.when(m == EARLY_V[q])
                def _():
                    start_down(q)

            return carry

        lax.fori_loop(0, rounds, up_step, 0)
        for q in range(len(early), col_chunks):
            start_down(q)
        lax.fori_loop(0, col_chunks, start_down_core, 0)

        def finish_rest(j, carry):
            finish_rows(j, 0, jnp.where(j == chunks - 1, 1, ROW_SPLIT))
            return carry

        lax.fori_loop(min(2 * (rounds - planes), chunks - 1), chunks, finish_rest, 0)
        shard_send.wait_send()

        def settle_up(j, carry):
            for piece in range(pieces):
                for stage in stages_from(piece, up_bits):
                    up_copy(j, piece, stage).wait_send()
            return carry

        lax.fori_loop(0, chunks, settle_up, 0)
        small[2].wait()
        db[...] = bias_row[...].reshape(1, own_width)
        small[3].wait()

        crossed = n_half * (slots - 1)
        entering = 2 * ((1 - n_half) * (slots - 1)) + 1 - n_half
        order = order_of(col_chunks, ROW_SPLIT, chunks)
        first_other = [k for k in range(len(order)) if order[k][0]][0]
        late_hidden = [(j, h) for h in range(1, ROW_SPLIT) for j in range(chunks)]

        def code_of(s):
            code = -1
            for k in range(len(order)):
                kind, q, h = order[k]
                code = jnp.where(s == k, kind * items + q * ROW_SPLIT + h, code)
            return code

        def lanes_of(u):
            return pl.ds(pl.multiple_of(u * slot_width, slot_width), slot_width)

        def sums(i, u, other):
            return ps.at[i // ROW_SPLIT + col_chunks * other, rows_of(i), lanes_of(u)]

        def z_copy(i, lane, src, up):
            return pltpu.make_async_remote_copy(
                src_ref=src, dst_ref=(zu if up else zd).at[lane, i],
                send_sem=z_send.at[lane, i], recv_sem=(zu_recv if up else zd_recv).at[lane, i],
                device_id={"tp": z + 1 if up else z - 1}, device_id_type=MESH)

        def final_copy(i, u):
            return pltpu.make_async_remote_copy(
                src_ref=sums(i, u, 1), dst_ref=fr.at[i], send_sem=f_send.at[i], recv_sem=f_recv.at[i],
                device_id=near(n_bit), device_id_type=MESH)

        def cross_copy(i):
            return pltpu.make_async_remote_copy(
                src_ref=sums(i, crossed, 1), dst_ref=cr.at[i], send_sem=c_send.at[i], recv_sem=c_recv.at[i],
                device_id=near(n_bit), device_id_type=MESH)

        def deliver(i, value):
            at = rows_of(i)
            for c in range(per_plane):
                place = pl.ds(pl.multiple_of(c * out_block + (i // ROW_SPLIT) * cols, cols), cols)
                total = ob[at, place].astype(jnp.float32) + value[:, pl.ds(c * cols, cols)].astype(jnp.float32)
                ob[at, place] = (total + db[:, place]).astype(jnp.bfloat16)

        def depth_of(to):
            above = planes - 1 - z
            return jnp.where(z < to, z, jnp.where(z > to, above, jnp.where(z > above, z, above)))

        def lane_source(i, lane):
            if lane < slots:
                return sums(i, lane, 0), 2 * lane + n_half
            if lane < 2 * slots - 1:
                u = lane - slots + 1 - n_half
                return sums(i, u, 1), 2 * u + n_half
            return cr.at[i], entering

        def chain(s, lane):
            _, to = lane_source(0, lane)
            late = CROSS_STEPS if lane == 2 * slots - 1 else 1
            code = code_of(s - late - HOP_STEPS * depth_of(to))
            i = code if lane < slots else code - items

            @pl.when((i >= 0) & (i < items))
            def _():
                src, _ = lane_source(i, lane)
                if lane == 2 * slots - 1:
                    cross_copy(i).wait_recv()

                @pl.when((z > 0) & (z <= to))
                def _():
                    z_copy(i, lane, src, True).wait_recv()
                    src[...] = (src[...].astype(jnp.float32) + zu[lane, i].astype(jnp.float32)).astype(jnp.bfloat16)

                @pl.when((z < planes - 1) & (z >= to))
                def _():
                    z_copy(i, lane, src, False).wait_recv()
                    src[...] = (src[...].astype(jnp.float32) + zd[lane, i].astype(jnp.float32)).astype(jnp.bfloat16)

                @pl.when(z < to)
                def _():
                    z_copy(i, lane, src, True).start()

                @pl.when(z > to)
                def _():
                    z_copy(i, lane, src, False).start()

                @pl.when(z == to)
                def _():
                    if slots <= lane < 2 * slots - 1:
                        final_copy(i, lane - slots + 1 - n_half).start()
                    else:
                        deliver(i, src)

        def down_dot(src, i, other):
            q = i // ROW_SPLIT
            ps[q + col_chunks * other, rows_of(i), pl.ds(0, cols * pieces)] = dot(src[rows_of(i), :], vb[q]).astype(jnp.bfloat16)

        def down_step(s, carry):
            code = code_of(s)
            i = code % items
            q = i // ROW_SPLIT
            own, other = (code >= 0) & (code < items), code >= items
            fresh = own & (i % ROW_SPLIT == 0)

            @pl.when(fresh)
            def _():
                for piece in range(1, pieces):
                    stages = stages_from(piece, down_bits)
                    if stages:
                        down_arrival(q, piece).wait_recv()
                        for stage in stages:
                            down_copy(q, piece, stage).start()
                        v_local(q, piece).start()
                v_local(q, 0).start()

            for lane in range(2 * slots):
                chain(s, lane)

            @pl.when(fresh)
            def _():
                for piece in range(1, pieces):
                    if not stages_from(piece, down_bits):
                        down_arrival(q, piece).wait_recv()
                        v_local(q, piece).start()
                for piece in range(pieces):
                    v_local(q, piece).wait()

            for h in range(1, ROW_SPLIT):
                @pl.when(s == 2 * h)
                def _():
                    finish(chunks - 1, h)

            @pl.when((s >= 2) & (s % 2 == 0) & (s < 2 + 2 * len(late_hidden)))
            def _():
                k = s // 2 - 1
                hidden_copy(k % chunks, k // chunks + 1).start()

            @pl.when(s == first_other)
            def _():
                for j in range(chunks):
                    for block in range(planes):
                        partial_copy(j, block).wait_send()

            @pl.when(other & (q == 0))
            def _():
                for j in range(chunks):
                    hidden_copy(j, i % ROW_SPLIT).wait_recv()

            @pl.when(own)
            def _():
                down_dot(hid, i, 0)

            @pl.when(other)
            def _():
                down_dot(hx, i, 1)
                cross_copy(i).start()
            return carry

        lax.fori_loop(0, 2 * items + HOP_STEPS * (planes - 1) + CROSS_STEPS, down_step, 0)

        @pl.when(z % 2 != n_half)
        def _():
            def body(i, carry):
                @pl.when(z != entering)
                def _():
                    final_copy(i, 0).wait_recv()
                    deliver(i, fr.at[i])
                return carry

            lax.fori_loop(0, items, body, 0)

        write = pltpu.make_async_copy(ob, out, misc_sem.at[0])
        write.start()

        def settle_down(q, carry):
            for piece in range(pieces):
                for stage in stages_from(piece, down_bits):
                    down_copy(q, piece, stage).wait_send()
            return carry

        lax.fori_loop(0, col_chunks, settle_down, 0)

        def settle_sums(i, carry):
            cross_copy(i).wait_send()
            for lane in range(2 * slots):
                src, to = lane_source(i, lane)

                @pl.when(z != to)
                def _():
                    z_copy(i, lane, src, True).wait_send()

                if slots <= lane < 2 * slots - 1:
                    @pl.when(z == to)
                    def _():
                        final_copy(i, lane - slots + 1 - n_half).wait_send()
            return carry

        lax.fori_loop(0, items, settle_sums, 0)

        def settle_hidden(j, carry):
            for h in range(ROW_SPLIT):
                hidden_copy(j, h).wait_send()
            return carry

        lax.fori_loop(0, chunks, settle_hidden, 0)
        for distance in range(planes - 1):
            @pl.when((z >= distance) & (z < planes - 1))
            def _():
                pass_on(distance, True).wait_send()

            @pl.when((z + distance <= planes - 1) & (z > 0))
            def _():
                pass_on(distance, False).wait_send()
        write.wait()

    def per_device(tokens, norm_gain, up_weight, up_bias, down_weight, down_bias):
        rows, width = tokens.shape
        depth, hidden = up_weight.shape
        out_block = down_weight.shape[1]
        own_width = down_bias.shape[0]
        hj = chunk_of(hidden, HID_CHUNK)
        cols = chunk_of(out_block, COL_CHUNK)
        chunks, col_chunks = hidden // hj, out_block // cols
        half, shard = width // 2, rows // planes
        slab = cols * pieces
        items, part = col_chunks * ROW_SPLIT, rows // ROW_SPLIT
        bf, f32 = jnp.bfloat16, jnp.float32
        dma = pltpu.SemaphoreType.DMA
        shared = (chunks, half, hj) == (col_chunks, hidden, slab)
        scratch = [
            pltpu.VMEM((2, shard, width), bf),
            pltpu.VMEM((shard, half), bf),
            pltpu.VMEM((rows, half), bf),
            pltpu.VMEM((rows, half), bf),
            pltpu.VMEM((chunks, half, hj), bf),
            pltpu.VMEM((max(chunks, 2 * col_chunks), rows, max(hj, slab)), bf),
            pltpu.VMEM((chunks, rows, hj), bf),
            pltpu.VMEM((part, hj), f32),
            pltpu.VMEM((rows, hidden), bf),
            pltpu.VMEM((rows, hidden), bf),
            pltpu.VMEM((2 * slots, items, part, per_plane * cols), bf),
            pltpu.VMEM((2 * slots, items, part, per_plane * cols), bf),
            pltpu.VMEM((items, part, per_plane * cols), bf),
            pltpu.VMEM((items, part, per_plane * cols), bf),
            pltpu.VMEM((rows, own_width), bf),
        ]
        if not shared:
            scratch.append(pltpu.VMEM((col_chunks, hidden, slab), bf))
        scratch += [
            pltpu.VMEM((1, width), bf),
            pltpu.VMEM((1, hidden), f32),
            pltpu.VMEM((1, own_width), f32),
            pltpu.VMEM((width,), bf),
            pltpu.VMEM((own_width,), f32),
            dma((2,)), dma((4,)), dma((chunks,)), dma((col_chunks, pieces)),
            dma((chunks, pieces - 1)), dma((chunks, pieces - 1)),
            dma((col_chunks, pieces - 1)), dma((col_chunks, pieces - 1)),
            dma, dma,
            dma((planes,)), dma((planes,)), dma((planes,)), dma((planes,)),
            dma((chunks, planes)), dma((chunks, planes)), dma((chunks, ROW_SPLIT)), dma((chunks, ROW_SPLIT)),
            dma((2 * slots, items)), dma((2 * slots, items)), dma((2 * slots, items)),
            dma((2, items)), dma((2, items)),
        ]
        hbm = pl.BlockSpec(memory_space=pltpu.HBM)
        result, _ = pl.pallas_call(
            kernel,
            out_shape=(
                jax.ShapeDtypeStruct((rows, own_width), bf),
                jax.ShapeDtypeStruct((col_chunks, hidden, slab), bf),
            ),
            in_specs=[hbm] * 6,
            out_specs=(hbm, hbm),
            scratch_shapes=scratch,
            compiler_params=pltpu.CompilerParams(
                collective_id=0, has_side_effects=True, vmem_limit_bytes=67043328),
        )(tokens, norm_gain, up_weight, up_bias[None, :], down_weight, down_bias)
        return result

    return per_device


def solution(mesh):
    in_specs = (P("grp", None), P(), P("grp", "tp"), P("tp"), P("tp", "grp"), P("tp"))
    return jax.shard_map(
        build(mesh.shape["grp"], mesh.shape["tp"]),
        mesh=mesh, in_specs=in_specs, out_specs=P("grp", "tp"), check_vma=False,
    )
```

```python
import functools

import jax
import jax.numpy as jnp
from jax import lax
from jax.experimental import pallas as pl
from jax.experimental.pallas import tpu as pltpu
from jax.sharding import PartitionSpec as P

MESH = pl.DeviceIdType.MESH
HID_CHUNK = 512
COL_CHUNK = 128
ROW_SPLIT = 2
HOP_STEPS = 2
DELIVER_STEPS = 8
CROSS_STEPS = 2
FIRST_HIDDEN = 1
EARLY_V = (-1, 1)


def chunk_of(extent, wanted):
    step = min(wanted, extent)
    while extent % step:
        step -= 128
    return step


def order_of(col_chunks, splits, chunks):
    def columns_at(q):
        return 0 if q < 2 else int(splits * (3.25 + 2 * (q - 2)))

    def hidden_at(h):
        return 2 + 2 * chunks * h if h else FIRST_HIDDEN * splits

    own = [(0, q, h) for h in range(splits) for q in range(min(2, col_chunks))]
    own += [(0, q, h) for q in range(2, col_chunks) for h in range(splits)]
    other = [(1, q, h) for q in range(col_chunks) for h in range(splits)]
    other.sort(key=lambda item: (max(columns_at(item[1]), hidden_at(item[2])), item[2], item[1]))
    order, loaded, load = [], set(), [0, 0]
    while own or other:
        here = len(order)
        known = [item for item in other if item[1] in loaded]
        ready = [item for item in known if max(columns_at(item[1]), hidden_at(item[2])) <= here]
        own_ready = own and columns_at(own[0][1]) <= here
        if own and (own_ready and (not ready or load[0] <= load[1]) or not (own_ready or ready)):
            pick = own.pop(0)
            loaded.add(pick[1])
        else:
            pick = (ready or known)[0]
            other.remove(pick)
        load[pick[0]] += 2
        load[1 - pick[0]] += 1
        order.append(pick)
    return order


def dot(a, b):
    return jnp.dot(a, b, preferred_element_type=jnp.float32)


def build(groups, planes):
    bits = groups.bit_length() - 1
    k_bit, n_bit = bits - 1, 1
    up_bits = [b for b in range(1, bits) if b != k_bit] + [0]
    down_bits = [b for b in range(bits - 1, 0, -1) if b != n_bit] + [0]
    per_plane = groups // planes
    pieces = groups // 2
    slots = planes // 2

    def masks_of(order):
        masks = [()]
        for bit in order:
            masks = masks + [m + (bit,) for m in masks]
        return masks

    up_masks, down_masks = masks_of(up_bits), masks_of(down_bits)

    def stages_from(piece, order):
        return [s for s in range(len(order)) if (1 << s) > piece]

    def kernel(
        tok, gain, w, ubias, v, dbias, out, vh,
        tk, sh, xo, xp, wb, ps, pr, acc, hid, hx, zu, zd, fr, cr, ob, *rest,
    ):
        rest = list(rest)
        vb = rest.pop(0) if len(rest) == 29 else wb
        (gv, ub, db, gain_row, bias_row, tk_sem, misc_sem, wl_sem, vl_sem,
         up_send, up_recv, dn_send, dn_recv, x_send, x_recv,
         zxu_send, zxu_recv, zxd_send, zxd_recv,
         p_send, p_recv, h_send, h_recv, z_send, zu_recv, zd_recv, f_sem, c_sem) = rest
        f_send, f_recv, c_send, c_recv = f_sem.at[0], f_sem.at[1], c_sem.at[0], c_sem.at[1]

        me = lax.axis_index("grp")
        z = lax.axis_index("tp")
        rows, width = tok.shape
        depth, hidden = w.shape
        out_block = v.shape[1]
        own_width = out.shape[1]
        half = width // 2
        chunks, _, hj = wb.shape
        cols = vb.shape[2] // pieces
        col_chunks = vb.shape[0]
        slot_width = per_plane * cols
        shard = rows // planes

        def bit_of(b):
            return (me // (1 << b)) % 2

        def flipped(index_bits):
            index = me
            for b in index_bits:
                index = index + (1 - 2 * bit_of(b)) * (1 << b)
            return index

        def near(b):
            return {"grp": flipped((b,))}

        k_half, n_half = bit_of(k_bit), bit_of(n_bit)

        def up_place(mask):
            return pl.multiple_of((flipped(mask) % pieces) * depth, depth)

        def down_place(mask):
            block = flipped(mask)
            return pl.multiple_of(((block // 4) * 2 + block % 2) * cols, cols)

        def up_copy(j, piece, stage):
            place = pl.ds(up_place(up_masks[piece]), depth)
            landing = wb.at[j, place, :]
            source = w.at[:, pl.ds(pl.multiple_of(j * hj, hj), hj)] if piece == 0 else landing
            slot = piece + (1 << stage) - 1
            return pltpu.make_async_remote_copy(
                src_ref=source, dst_ref=landing,
                send_sem=up_send.at[j, slot], recv_sem=up_recv.at[j, slot],
                device_id=near(up_bits[stage]), device_id_type=MESH)

        def up_arrival(j, piece):
            place = pl.ds(up_place(up_masks[piece]), depth)
            landing = wb.at[j, place, :]
            stage = piece.bit_length() - 1
            return pltpu.make_async_remote_copy(
                src_ref=landing, dst_ref=landing,
                send_sem=up_send.at[j, piece - 1], recv_sem=up_recv.at[j, piece - 1],
                device_id=near(up_bits[stage]), device_id_type=MESH)

        def w_local(j):
            return pltpu.make_async_copy(
                w.at[:, pl.ds(pl.multiple_of(j * hj, hj), hj)],
                wb.at[j, pl.ds(up_place(()), depth), :], wl_sem.at[j])

        def down_copy(q, piece, stage):
            place = pl.ds(down_place(down_masks[piece]), cols)
            landing = vh.at[q, :, place]
            source = v.at[:, pl.ds(pl.multiple_of(q * cols, cols), cols)] if piece == 0 else landing
            slot = piece + (1 << stage) - 1
            return pltpu.make_async_remote_copy(
                src_ref=source, dst_ref=landing,
                send_sem=dn_send.at[q, slot], recv_sem=dn_recv.at[q, slot],
                device_id=near(down_bits[stage]), device_id_type=MESH)

        def down_arrival(q, piece):
            landing = vh.at[q, :, pl.ds(down_place(down_masks[piece]), cols)]
            stage = piece.bit_length() - 1
            return pltpu.make_async_remote_copy(
                src_ref=landing, dst_ref=landing,
                send_sem=dn_send.at[q, piece - 1], recv_sem=dn_recv.at[q, piece - 1],
                device_id=near(down_bits[stage]), device_id_type=MESH)

        def v_local(q, piece):
            place = pl.ds(down_place(down_masks[piece]), cols)
            source = v.at[:, pl.ds(pl.multiple_of(q * cols, cols), cols)] if piece == 0 else vh.at[q, :, place]
            return pltpu.make_async_copy(source, vb.at[q, :, place], vl_sem.at[q, piece])

        barrier = pltpu.get_barrier_semaphore()
        for b in range(bits):
            pl.semaphore_signal(barrier, inc=1, device_id=near(b), device_id_type=MESH)

        @pl.when(z > 0)
        def _():
            pl.semaphore_signal(barrier, inc=1, device_id={"tp": z - 1}, device_id_type=MESH)

        @pl.when(z < planes - 1)
        def _():
            pl.semaphore_signal(barrier, inc=1, device_id={"tp": z + 1}, device_id_type=MESH)

        shard_rows = pl.ds(pl.multiple_of(z * shard, shard), shard)

        def token_copy(index, slot):
            source = shard_rows if index < 0 else pl.ds(index * shard, shard)
            return pltpu.make_async_copy(tok.at[source, :], tk.at[slot], tk_sem.at[slot])

        token_copy(-1, 0).start()
        token_copy(0, 1).start()
        small = [
            pltpu.make_async_copy(gain, gain_row, misc_sem.at[0]),
            pltpu.make_async_copy(ubias, ub, misc_sem.at[1]),
            pltpu.make_async_copy(dbias, bias_row, misc_sem.at[2]),
            pltpu.make_async_copy(
                tok.at[:, pl.ds(pl.multiple_of(z * own_width, own_width), own_width)], ob, misc_sem.at[3]),
        ]
        for copy in small:
            copy.start()

        neighbours = bits + jnp.where(z > 0, 1, 0) + jnp.where(z < planes - 1, 1, 0)
        pl.semaphore_wait(barrier, neighbours)

        def start_up(j, carry):
            for stage in range(len(up_bits)):
                up_copy(j, 0, stage).start()
            w_local(j).start()
            return carry

        lax.fori_loop(0, chunks, start_up, 0)
        small[0].wait()
        gv[...] = gain_row[...].reshape(1, width)

        tile = 16

        def normalise(slot, column, dst, base):
            def body(i, carry):
                at = pl.multiple_of(i * tile, tile)
                values = tk[slot, pl.ds(at, tile), :].astype(jnp.float32)
                centre = jnp.mean(values, axis=1, keepdims=True)
                shifted = values - centre
                scale = lax.rsqrt(jnp.mean(shifted * shifted, axis=1, keepdims=True) + 1e-06)
                part = tk[slot, pl.ds(at, tile), pl.ds(column, half)].astype(jnp.float32)
                normed = (part - centre) * scale * gv[:, pl.ds(column, half)].astype(jnp.float32)
                dst[pl.ds(pl.multiple_of(base + at, tile), tile), :] = normed.astype(jnp.bfloat16)
                return carry

            lax.fori_loop(0, shard // tile, body, 0)

        own_column = pl.multiple_of(k_half * half, half)
        other_column = pl.multiple_of((1 - k_half) * half, half)

        token_copy(-1, 0).wait()
        normalise(0, other_column, sh, 0)
        shard_send = pltpu.make_async_remote_copy(
            src_ref=sh, dst_ref=xp.at[shard_rows, :],
            send_sem=x_send, recv_sem=x_recv, device_id=near(k_bit), device_id_type=MESH)
        shard_send.start()

        def start_down(q):
            down_copy(q, 0, 0).start()

        early = [q for q in range(len(EARLY_V)) if q < col_chunks]
        for q in early:
            if EARLY_V[q] < 0:
                start_down(q)

        def start_down_core(q, carry):
            for stage in range(1, len(down_bits)):
                down_copy(q, 0, stage).start()
            return carry

        for c in range(planes):
            slot = (c + 1) % 2
            if c + 1 < planes:
                token_copy(c + 1, 1 - slot).start()
            token_copy(c, slot).wait()
            normalise(slot, own_column, xo, c * shard)

        def pass_on(distance, rising):
            source = z - distance if rising else z + distance
            place = pl.ds(pl.multiple_of(source * shard, shard), shard)
            return pltpu.make_async_remote_copy(
                src_ref=xp.at[place, :], dst_ref=xp.at[place, :],
                send_sem=(zxu_send if rising else zxd_send).at[distance],
                recv_sem=(zxu_recv if rising else zxd_recv).at[distance],
                device_id={"tp": z + 1 if rising else z - 1}, device_id_type=MESH)

        def arrival(distance, rising):
            source = z - distance if rising else z + distance
            place = pl.ds(pl.multiple_of(source * shard, shard), shard)
            return pltpu.make_async_remote_copy(
                src_ref=xp.at[place, :], dst_ref=xp.at[place, :],
                send_sem=(zxu_send if rising else zxd_send).at[distance - 1],
                recv_sem=(zxu_recv if rising else zxd_recv).at[distance - 1],
                device_id={"tp": z - 1 if rising else z + 1}, device_id_type=MESH)

        def pass_tokens(distance):
            @pl.when(distance == 0)
            def _():
                shard_send.wait_recv()

            @pl.when((distance > 0) & (z >= distance))
            def _():
                arrival(distance, True).wait_recv()

            @pl.when((distance > 0) & (z + distance <= planes - 1))
            def _():
                arrival(distance, False).wait_recv()

            @pl.when((z >= distance) & (z < planes - 1) & (distance < planes - 1))
            def _():
                pass_on(distance, True).start()

            @pl.when((z + distance <= planes - 1) & (z > 0) & (distance < planes - 1))
            def _():
                pass_on(distance, False).start()

        small[1].wait()

        parked = ps.shape[0] - chunks

        def partial_copy(j, block):
            place = pl.ds(pl.multiple_of(block * shard, shard), shard)
            return pltpu.make_async_remote_copy(
                src_ref=ps.at[parked + j, place, pl.ds(0, hj)], dst_ref=pr.at[j, place, :],
                send_sem=p_send.at[j, block], recv_sem=p_recv.at[j, block],
                device_id=near(k_bit), device_id_type=MESH)

        part = rows // ROW_SPLIT
        items = col_chunks * ROW_SPLIT

        def rows_of(i):
            return pl.ds(pl.multiple_of((i % ROW_SPLIT) * part, part), part)

        def hidden_copy(j, h):
            place = pl.ds(pl.multiple_of(j * hj, hj), hj)
            return pltpu.make_async_remote_copy(
                src_ref=hid.at[rows_of(h), place], dst_ref=hx.at[rows_of(h), place],
                send_sem=h_send.at[j, h], recv_sem=h_recv.at[j, h],
                device_id=near(n_bit), device_id_type=MESH)

        row_tile = min(256, rows)

        def finish(j, h):
            place = pl.ds(pl.multiple_of(j * hj, hj), hj)
            acc[...] = dot(xo[rows_of(h), :], wb[j])
            for block in range(planes // ROW_SPLIT):
                partial_copy(j, h * (planes // ROW_SPLIT) + block).wait_recv()
            pre = acc[...] + pr[j, rows_of(h), :].astype(jnp.float32) + ub[:, place]
            hid[rows_of(h), place] = jax.nn.gelu(pre, approximate=True).astype(jnp.bfloat16)

            @pl.when(h == 0)
            def _():
                hidden_copy(j, 0).start()

        def finish_rows(j, first, last):
            def body(h, carry):
                finish(j, h)
                return carry

            lax.fori_loop(first, last, body, 0)

        rounds = max(planes, chunks)

        def up_step(m, carry):
            for j in range(2):
                @pl.when((m >= planes) & (2 * (m - planes) + j < chunks - 1))
                def _():
                    finish_rows(2 * (m - planes) + j, 0, ROW_SPLIT)

            @pl.when(m < chunks)
            def _():
                for piece in range(1, pieces):
                    stages = stages_from(piece, up_bits)
                    if stages:
                        up_arrival(m, piece).wait_recv()
                        for stage in stages:
                            up_copy(m, piece, stage).start()

            @pl.when(m < planes)
            def _():
                pass_tokens(m)

            @pl.when(m < chunks)
            def _():
                for piece in range(1, pieces):
                    if not stages_from(piece, up_bits):
                        up_arrival(m, piece).wait_recv()
                w_local(m).wait()

            def sent(t, carry):
                distance = jnp.where(t // 2 < m, t // 2, m)
                j = jnp.where(t // 2 <= m, m, t // 2 - m - 1)
                block = jnp.where(t % 2 == 0, z - distance, z + distance)
                straight = m >= planes
                block = jnp.where(straight, t, block)
                j = jnp.where(straight, m, j)

                @pl.when((block >= 0) & (block < planes) & (j < chunks) & (straight | (t % 2 == 0) | (distance > 0)))
                def _():
                    at = pl.ds(pl.multiple_of(block * shard, shard), shard)
                    ps[parked + j, at, pl.ds(0, hj)] = dot(xp[at, :], wb[j]).astype(jnp.bfloat16)
                    partial_copy(j, block).start()
                return carry

            lax.fori_loop(0, 2 * (2 * m + 1), sent, 0)
            for q in early:
                @pl.when(m == EARLY_V[q])
                def _():
                    start_down(q)

            return carry

        lax.fori_loop(0, rounds, up_step, 0)
        for q in range(len(early), col_chunks):
            start_down(q)
        lax.fori_loop(0, col_chunks, start_down_core, 0)

        def finish_rest(j, carry):
            finish_rows(j, 0, jnp.where(j == chunks - 1, 1, ROW_SPLIT))
            return carry

        lax.fori_loop(min(2 * (rounds - planes), chunks - 1), chunks, finish_rest, 0)
        shard_send.wait_send()

        def settle_up(j, carry):
            for piece in range(pieces):
                for stage in stages_from(piece, up_bits):
                    up_copy(j, piece, stage).wait_send()
            return carry

        lax.fori_loop(0, chunks, settle_up, 0)
        small[2].wait()
        db[...] = bias_row[...].reshape(1, own_width)
        small[3].wait()

        crossed = n_half * (slots - 1)
        entering = 2 * ((1 - n_half) * (slots - 1)) + 1 - n_half
        order = order_of(col_chunks, ROW_SPLIT, chunks)
        first_other = [k for k in range(len(order)) if order[k][0]][0]
        late_hidden = [(j, h) for h in range(1, ROW_SPLIT) for j in range(chunks)]

        def code_of(s):
            code = -1
            for k in range(len(order)):
                kind, q, h = order[k]
                code = jnp.where(s == k, kind * items + q * ROW_SPLIT + h, code)
            return code

        def lanes_of(u):
            return pl.ds(pl.multiple_of(u * slot_width, slot_width), slot_width)

        def sums(i, u, other):
            return ps.at[i // ROW_SPLIT + col_chunks * other, rows_of(i), lanes_of(u)]

        def z_copy(i, lane, src, up):
            return pltpu.make_async_remote_copy(
                src_ref=src, dst_ref=(zu if up else zd).at[lane, i],
                send_sem=z_send.at[lane, i], recv_sem=(zu_recv if up else zd_recv).at[lane, i],
                device_id={"tp": z + 1 if up else z - 1}, device_id_type=MESH)

        def final_copy(i, u):
            return pltpu.make_async_remote_copy(
                src_ref=sums(i, u, 1), dst_ref=fr.at[i], send_sem=f_send.at[i], recv_sem=f_recv.at[i],
                device_id=near(n_bit), device_id_type=MESH)

        def cross_copy(i):
            return pltpu.make_async_remote_copy(
                src_ref=sums(i, crossed, 1), dst_ref=cr.at[i], send_sem=c_send.at[i], recv_sem=c_recv.at[i],
                device_id=near(n_bit), device_id_type=MESH)

        def deliver(i, value):
            at = rows_of(i)
            for c in range(per_plane):
                place = pl.ds(pl.multiple_of(c * out_block + (i // ROW_SPLIT) * cols, cols), cols)
                total = ob[at, place].astype(jnp.float32) + value[:, pl.ds(c * cols, cols)].astype(jnp.float32)
                ob[at, place] = (total + db[:, place]).astype(jnp.bfloat16)

        def depth_of(to):
            above = planes - 1 - z
            return jnp.where(z < to, z, jnp.where(z > to, above, jnp.where(z > above, z, above)))

        def lane_source(i, lane):
            if lane < slots:
                return sums(i, lane, 0), 2 * lane + n_half
            if lane < 2 * slots - 1:
                u = lane - slots + 1 - n_half
                return sums(i, u, 1), 2 * u + n_half
            return cr.at[i], entering

        def chain(s, lane):
            _, to = lane_source(0, lane)
            late = CROSS_STEPS if lane == 2 * slots - 1 else 1
            code = code_of(s - late - HOP_STEPS * depth_of(to))
            i = code if lane < slots else code - items

            @pl.when((i >= 0) & (i < items))
            def _():
                src, _ = lane_source(i, lane)
                if lane == 2 * slots - 1:
                    cross_copy(i).wait_recv()

                @pl.when((z > 0) & (z <= to))
                def _():
                    z_copy(i, lane, src, True).wait_recv()
                    src[...] = (src[...].astype(jnp.float32) + zu[lane, i].astype(jnp.float32)).astype(jnp.bfloat16)

                @pl.when((z < planes - 1) & (z >= to))
                def _():
                    z_copy(i, lane, src, False).wait_recv()
                    src[...] = (src[...].astype(jnp.float32) + zd[lane, i].astype(jnp.float32)).astype(jnp.bfloat16)

                @pl.when(z < to)
                def _():
                    z_copy(i, lane, src, True).start()

                @pl.when(z > to)
                def _():
                    z_copy(i, lane, src, False).start()

                @pl.when(z == to)
                def _():
                    if slots <= lane < 2 * slots - 1:
                        final_copy(i, lane - slots + 1 - n_half).start()
                    else:
                        deliver(i, src)

        def take_final(s):
            i = code_of(s - DELIVER_STEPS) - items

            @pl.when((i >= 0) & (z % 2 != n_half) & (z != entering))
            def _():
                final_copy(i, 0).wait_recv()
                deliver(i, fr.at[i])

        def down_dot(src, i, other):
            q = i // ROW_SPLIT
            ps[q + col_chunks * other, rows_of(i), pl.ds(0, cols * pieces)] = dot(src[rows_of(i), :], vb[q]).astype(jnp.bfloat16)

        def down_step(s, carry):
            code = code_of(s)
            i = code % items
            q = i // ROW_SPLIT
            own, other = (code >= 0) & (code < items), code >= items
            fresh = own & (i % ROW_SPLIT == 0)

            @pl.when(fresh)
            def _():
                for piece in range(1, pieces):
                    stages = stages_from(piece, down_bits)
                    if stages:
                        down_arrival(q, piece).wait_recv()
                        for stage in stages:
                            down_copy(q, piece, stage).start()
                        v_local(q, piece).start()
                v_local(q, 0).start()

            for lane in range(2 * slots):
                chain(s, lane)
            take_final(s)

            @pl.when(fresh)
            def _():
                for piece in range(1, pieces):
                    if not stages_from(piece, down_bits):
                        down_arrival(q, piece).wait_recv()
                        v_local(q, piece).start()
                for piece in range(pieces):
                    v_local(q, piece).wait()

            for h in range(1, ROW_SPLIT):
                @pl.when(s == 2 * h)
                def _():
                    finish(chunks - 1, h)

            @pl.when((s >= 2) & (s % 2 == 0) & (s < 2 + 2 * len(late_hidden)))
            def _():
                k = s // 2 - 1
                hidden_copy(k % chunks, k // chunks + 1).start()

            @pl.when(s == first_other)
            def _():
                for j in range(chunks):
                    for block in range(planes):
                        partial_copy(j, block).wait_send()

            @pl.when(other & (q == 0))
            def _():
                for j in range(chunks):
                    hidden_copy(j, i % ROW_SPLIT).wait_recv()

            @pl.when(own)
            def _():
                down_dot(hid, i, 0)

            @pl.when(other)
            def _():
                down_dot(hx, i, 1)
                cross_copy(i).start()
            return carry

        lax.fori_loop(0, 2 * items + max(HOP_STEPS * (planes - 1) + CROSS_STEPS, DELIVER_STEPS), down_step, 0)

        write = pltpu.make_async_copy(ob, out, misc_sem.at[0])
        write.start()

        def settle_down(q, carry):
            for piece in range(pieces):
                for stage in stages_from(piece, down_bits):
                    down_copy(q, piece, stage).wait_send()
            return carry

        lax.fori_loop(0, col_chunks, settle_down, 0)

        def settle_sums(i, carry):
            cross_copy(i).wait_send()
            for lane in range(2 * slots):
                src, to = lane_source(i, lane)

                @pl.when(z != to)
                def _():
                    z_copy(i, lane, src, True).wait_send()

                if slots <= lane < 2 * slots - 1:
                    @pl.when(z == to)
                    def _():
                        final_copy(i, lane - slots + 1 - n_half).wait_send()
            return carry

        lax.fori_loop(0, items, settle_sums, 0)

        def settle_hidden(j, carry):
            for h in range(ROW_SPLIT):
                hidden_copy(j, h).wait_send()
            return carry

        lax.fori_loop(0, chunks, settle_hidden, 0)
        for distance in range(planes - 1):
            @pl.when((z >= distance) & (z < planes - 1))
            def _():
                pass_on(distance, True).wait_send()

            @pl.when((z + distance <= planes - 1) & (z > 0))
            def _():
                pass_on(distance, False).wait_send()
        write.wait()

    def per_device(tokens, norm_gain, up_weight, up_bias, down_weight, down_bias):
        rows, width = tokens.shape
        depth, hidden = up_weight.shape
        out_block = down_weight.shape[1]
        own_width = down_bias.shape[0]
        hj = chunk_of(hidden, HID_CHUNK)
        cols = chunk_of(out_block, COL_CHUNK)
        chunks, col_chunks = hidden // hj, out_block // cols
        half, shard = width // 2, rows // planes
        slab = cols * pieces
        items, part = col_chunks * ROW_SPLIT, rows // ROW_SPLIT
        bf, f32 = jnp.bfloat16, jnp.float32
        dma = pltpu.SemaphoreType.DMA
        shared = (chunks, half, hj) == (col_chunks, hidden, slab)
        scratch = [
            pltpu.VMEM((2, shard, width), bf),
            pltpu.VMEM((shard, half), bf),
            pltpu.VMEM((rows, half), bf),
            pltpu.VMEM((rows, half), bf),
            pltpu.VMEM((chunks, half, hj), bf),
            pltpu.VMEM((max(chunks, 2 * col_chunks), rows, max(hj, slab)), bf),
            pltpu.VMEM((chunks, rows, hj), bf),
            pltpu.VMEM((part, hj), f32),
            pltpu.VMEM((rows, hidden), bf),
            pltpu.VMEM((rows, hidden), bf),
            pltpu.VMEM((2 * slots, items, part, per_plane * cols), bf),
            pltpu.VMEM((2 * slots, items, part, per_plane * cols), bf),
            pltpu.VMEM((items, part, per_plane * cols), bf),
            pltpu.VMEM((items, part, per_plane * cols), bf),
            pltpu.VMEM((rows, own_width), bf),
        ]
        if not shared:
            scratch.append(pltpu.VMEM((col_chunks, hidden, slab), bf))
        scratch += [
            pltpu.VMEM((1, width), bf),
            pltpu.VMEM((1, hidden), f32),
            pltpu.VMEM((1, own_width), f32),
            pltpu.VMEM((width,), bf),
            pltpu.VMEM((own_width,), f32),
            dma((2,)), dma((4,)), dma((chunks,)), dma((col_chunks, pieces)),
            dma((chunks, pieces - 1)), dma((chunks, pieces - 1)),
            dma((col_chunks, pieces - 1)), dma((col_chunks, pieces - 1)),
            dma, dma,
            dma((planes,)), dma((planes,)), dma((planes,)), dma((planes,)),
            dma((chunks, planes)), dma((chunks, planes)), dma((chunks, ROW_SPLIT)), dma((chunks, ROW_SPLIT)),
            dma((2 * slots, items)), dma((2 * slots, items)), dma((2 * slots, items)),
            dma((2, items)), dma((2, items)),
        ]
        hbm = pl.BlockSpec(memory_space=pltpu.HBM)
        result, _ = pl.pallas_call(
            kernel,
            out_shape=(
                jax.ShapeDtypeStruct((rows, own_width), bf),
                jax.ShapeDtypeStruct((col_chunks, hidden, slab), bf),
            ),
            in_specs=[hbm] * 6,
            out_specs=(hbm, hbm),
            scratch_shapes=scratch,
            compiler_params=pltpu.CompilerParams(
                collective_id=0, has_side_effects=True, vmem_limit_bytes=67043328),
        )(tokens, norm_gain, up_weight, up_bias[None, :], down_weight, down_bias)
        return result

    return per_device


def solution(mesh):
    in_specs = (P("grp", None), P(), P("grp", "tp"), P("tp"), P("tp", "grp"), P("tp"))
    return jax.shard_map(
        build(mesh.shape["grp"], mesh.shape["tp"]),
        mesh=mesh, in_specs=in_specs, out_specs=P("grp", "tp"), check_vma=False,
    )
```
